32 devices in a mesh: expert: 4 (over x, core), dp: 8 (over z, y).
Axes of the slice: x: 2, y: 2, z: 4, core: 2. Of those that a mesh axis runs over, the one named last changes fastest.
Arguments:
- tokens: bfloat16 [4096, 1024], P(('expert', 'dp')), may hold values from -6 to 6
- norm_gain: float32 [1024], replicated, may hold values from 0.1 to 1.9
- router_weight: bfloat16 [1024, 4], replicated, may hold values from -0.3984375 to 0.3984375
- shared_gate_vector: float32 [1024], replicated, may hold values from -0.4 to 0.4
- expert_ids: int32 [4096, 2], P(('expert', 'dp')), may hold values from 0 to 3, all different within a row; in each aligned block of 128 rows (0 to 127, 128 to 255, ...) at most 96 rows name the same one
- gate_weight: bfloat16 [4, 1024, 4096], P('expert', None, 'dp'), may hold values from -0.1875 to 0.1875
- up_weight: bfloat16 [4, 1024, 4096], P('expert', None, 'dp'), may hold values from -0.1875 to 0.1875
- down_weight: bfloat16 [4, 1024, 4096], P('expert', None, 'dp'), may hold values from -0.09375 to 0.09375
- shared_gate_weight: bfloat16 [1024, 4096], P(None, 'expert'), may hold values from -0.1875 to 0.1875
- shared_up_weight: bfloat16 [1024, 4096], P(None, 'expert'), may hold values from -0.1875 to 0.1875
- shared_down_weight: bfloat16 [4096, 1024], P('expert'), may hold values from -0.09375 to 0.09375
Outputs:
- mixed: bfloat16 [4096, 1024], P(('expert', 'dp'))
The draws below stay inside these ranges and needn't reach their ends.
Inputs may be any that keep to these rules, and one draw needn't show every extreme that they name: `expert_ids`: in each aligned block of 128 rows (the rows of one device) no expert is named by more than 96 pairs, and in some block one expert is named by exactly 96; the two ids of a row differ.
All inputs are finite; a program needn't handle non-finite values.
Results may differ from the reference program's by a relative error of at most 0.0085.
Values may be sent and summed in bfloat16 or wider, within the bound.
A program may use at most 128 MiB of HBM per device.

```python
import math
import jax
import jax.numpy as jnp
import numpy as np
from jax import lax

D = 1024
FF = 4096
SFF = 4096
TOK_DEV = 128
EXPERTS = 4
CAP = 96
TOKENS = 4096
N_EXPERT = 4


def shard_levels(stream_key, extent, shards, least, top_value):
    factor_of = 1.0
    for axis_at, parts in shards:
        steps = jax.random.uniform(jax.random.fold_in(jax.random.fold_in(stream_key, 6), axis_at), (parts,), jnp.float32, least / len(shards), top_value / len(shards))
        factor_of = factor_of * jnp.repeat(jnp.exp(steps), extent[axis_at] // parts).reshape((-1,) + (1,) * (len(extent) - 1 - axis_at))
    return factor_of


def routed_block(rng, own, number, rows, count, top, reach, skew):
    sequence = jax.random.permutation(rng, count)
    heavy_load, common = shares(count, rows * top, reach, skew, True), shares(count, rows * top, reach, skew, False)
    places = jnp.arange(count)

    def named(tallies, rotation):
        used = int((tallies > 0).sum())
        fixed = max(1, used // 4)
        shifted = fixed + (places - fixed + rotation * (used - fixed)) % max(1, count - fixed)
        return jnp.zeros((count,), jnp.int32).at[sequence[jnp.where(places < fixed, places, shifted)]].set(jnp.asarray(tallies, jnp.int32))

    tallies = jnp.where(number % 4 == 0, named(heavy_load, number // 4), named(common, number - number // 4 - 1))
    mixed = jax.random.permutation(jax.random.fold_in(own, 3), count)
    donor, receiver = mixed[0:count // 2 * 2:2], mixed[1:count // 2 * 2:2]
    room = jnp.minimum(tallies[donor] - 1, reach - tallies[receiver]) // 2
    room = jnp.where((donor == sequence[0]) | (receiver == sequence[0]) | (tallies[receiver] == 0), 0, jnp.maximum(room, 0))
    shifted = jax.random.randint(jax.random.fold_in(own, 4), (count // 2,), 0, 1 << 20) % (room + 1)
    tallies = tallies.at[donor].add(-shifted).at[receiver].add(shifted)
    items = jnp.searchsorted(jnp.cumsum(tallies), jnp.arange(rows * top), side="right").astype(jnp.int32)
    listing = items.reshape(top, rows).T
    listing = listing[jax.random.permutation(jax.random.fold_in(own, 1), rows)]
    rotation = jax.random.randint(jax.random.fold_in(own, 2), (rows, 1), 0, top)
    return jnp.take_along_axis(listing, (jnp.arange(top)[None, :] + rotation) % top, axis=1)


def shares(number_of, total, bound, lean, full):
    portions = [(1 << 20) // math.isqrt(rank ** lean) + 1 for rank in range(1, number_of + 1)]
    largest = bound if full else min(bound, max(-(-total // number_of), total * portions[0] // sum(portions)))
    least = 1 if total - largest >= number_of - 1 else 0
    holding, surplus = [largest] + [least] * (number_of - 1), total - largest - least * (number_of - 1)
    while surplus > 0:
        movable = [i for i in range(1, number_of) if holding[i] < largest] or [i for i in range(1, number_of) if holding[i] < bound]
        mass, remaining = sum([portions[i] for i in movable]), surplus
        for i in movable:
            addition = min(bound - holding[i], max(1, remaining * portions[i] // mass), surplus)
            holding[i] = holding[i] + addition
            surplus = surplus - addition
    return np.array(holding)


def bell_draw(own_key, shape, spread, limit, cuts=(), kind=jnp.bfloat16):
    values = spread * jax.random.normal(own_key, shape, jnp.float32)
    if cuts:
        values = values * shard_levels(own_key, shape, cuts, -0.22, 0.18)
    return jnp.clip(values, -limit, limit).astype(kind)


def setup_inputs(seed: int = 0) -> dict:
    arg_keys = jax.random.split(jax.random.key(seed), 12)
    tokens = bell_draw(arg_keys[0], (TOKENS, D), 1.0, 6.0, ((0, 32),))
    norm_gain = jnp.clip(1.0 + 0.18 * jax.random.normal(arg_keys[1], (D,), jnp.float32), 0.1, 1.9)
    router_weight = bell_draw(arg_keys[2], (D, EXPERTS), 0.0625, 0.3984375)
    shared_gate_vector = bell_draw(arg_keys[3], (D,), 0.0625, 0.4, (), jnp.float32)
    expert_ids_keys = jax.random.split(jax.random.fold_in(arg_keys[4], 1), TOKENS // TOK_DEV)
    expert_ids_turns = jax.random.permutation(jax.random.fold_in(arg_keys[4], 3), TOKENS // TOK_DEV)
    expert_ids = jax.vmap(lambda own, number: routed_block(jax.random.fold_in(arg_keys[4], 2), own, number, TOK_DEV, EXPERTS, 2, CAP, 2))(expert_ids_keys, expert_ids_turns).reshape((TOKENS, 2))
    gate_weight = bell_draw(arg_keys[5], (EXPERTS, D, FF), D ** -0.5, 0.1875, ((0, 4), (2, 8)))
    up_weight = bell_draw(arg_keys[6], (EXPERTS, D, FF), D ** -0.5, 0.1875, ((0, 4), (2, 8)))
    down_weight = bell_draw(arg_keys[7], (EXPERTS, D, FF), FF ** -0.5, 0.09375, ((0, 4), (2, 8)))
    shared_gate_weight = bell_draw(arg_keys[8], (D, SFF), D ** -0.5, 0.1875, ((1, 4),))
    shared_up_weight = bell_draw(arg_keys[9], (D, SFF), D ** -0.5, 0.1875, ((1, 4),))
    shared_down_weight = bell_draw(arg_keys[10], (SFF, D), SFF ** -0.5, 0.09375, ((0, 4),))
    return dict(tokens=tokens, norm_gain=norm_gain, router_weight=router_weight, shared_gate_vector=shared_gate_vector, expert_ids=expert_ids, gate_weight=gate_weight, up_weight=up_weight, down_weight=down_weight, shared_gate_weight=shared_gate_weight, shared_up_weight=shared_up_weight, shared_down_weight=shared_down_weight)


def rms_norm(values, gain):
    floats = values.astype(jnp.float32)
    mean_square = lax.optimization_barrier(jnp.mean(floats * floats, axis=-1, keepdims=True))
    return (floats * lax.rsqrt(mean_square + 1e-06) * gain).astype(jnp.bfloat16)

def routing(normed, router_weight, expert_ids):
    logits = jnp.dot(normed, router_weight, preferred_element_type=jnp.float32)
    onehot = expert_ids[:, :, None] == jnp.arange(router_weight.shape[1], dtype=jnp.int32)[None, None, :]
    picked = lax.optimization_barrier(jnp.sum(jnp.where(onehot, logits[:, None, :], jnp.float32(0.0)), axis=-1))
    first_weight = jax.nn.sigmoid(picked[:, 0] - picked[:, 1])
    return jnp.stack([first_weight, 1.0 - first_weight], axis=1)

def slot_of(block_ids):
    flat_ids = block_ids.reshape(-1)
    onehot = (flat_ids[:, None] == jnp.arange(EXPERTS, dtype=jnp.int32)[None, :]).astype(jnp.int32)
    before = jnp.cumsum(onehot, axis=0) - onehot
    return lax.optimization_barrier(jnp.sum(before * onehot, axis=1)).reshape(block_ids.shape).astype(jnp.int32)

def reference(tokens, norm_gain, router_weight, shared_gate_vector, expert_ids, gate_weight, up_weight, down_weight, shared_gate_weight, shared_up_weight, shared_down_weight):
    normed = rms_norm(tokens, norm_gain)
    route_weight = routing(normed, router_weight, expert_ids)
    num_blocks = TOKENS // TOK_DEV
    slot = jax.vmap(slot_of)(expert_ids.reshape(num_blocks, TOK_DEV, 2)).reshape(TOKENS, 2)
    source_block = (jnp.arange(TOKENS, dtype=jnp.int32) // TOK_DEV).astype(jnp.int32)
    position = (source_block[:, None] * CAP + slot).astype(jnp.int32)
    padded_rows = num_blocks * CAP

    def expert_step(running, expert_index):
        slot_index = jnp.where(expert_ids == expert_index, position, padded_rows).astype(jnp.int32)
        buffer = jnp.zeros((padded_rows, D), jnp.bfloat16)
        buffer = buffer.at[slot_index[:, 0]].set(normed, mode='drop')
        buffer = buffer.at[slot_index[:, 1]].set(normed, mode='drop')
        gate_part = jnp.dot(buffer, gate_weight[expert_index], preferred_element_type=jnp.float32)
        up_part = jnp.dot(buffer, up_weight[expert_index], preferred_element_type=jnp.float32)
        hidden = (jax.nn.silu(gate_part) * up_part).astype(jnp.bfloat16)
        expert_out = lax.dot_general(hidden, down_weight[expert_index], (((1,), (1,)), ((), ())), preferred_element_type=jnp.float32).astype(jnp.bfloat16)
        for column in range(2):
            fetched = expert_out[jnp.minimum(slot_index[:, column], padded_rows - 1)].astype(jnp.float32)
            scale = jnp.where(expert_ids[:, column] == expert_index, route_weight[:, column], jnp.float32(0.0))
            running = running + scale[:, None] * fetched
        return (running, None)
    routed, _ = lax.scan(expert_step, jnp.zeros((TOKENS, D), jnp.float32), jnp.arange(EXPERTS, dtype=jnp.int32))
    block_units = SFF // N_EXPERT
    shared = jnp.zeros((TOKENS, D), jnp.float32)
    for block_index in range(N_EXPERT):
        lower = block_index * block_units
        gate_part = jnp.dot(normed, shared_gate_weight[:, lower:lower + block_units], preferred_element_type=jnp.float32)
        up_part = jnp.dot(normed, shared_up_weight[:, lower:lower + block_units], preferred_element_type=jnp.float32)
        hidden = (jax.nn.silu(gate_part) * up_part).astype(jnp.bfloat16)
        partial_out = jnp.dot(hidden, shared_down_weight[lower:lower + block_units, :], preferred_element_type=jnp.float32).astype(jnp.bfloat16)
        partial_out = lax.optimization_barrier(partial_out)
        shared = shared + partial_out.astype(jnp.float32)
    shared_gate = jax.nn.sigmoid(lax.optimization_barrier(jnp.sum(normed.astype(jnp.float32) * shared_gate_vector, axis=-1)))
    return (routed + shared_gate[:, None] * shared).astype(jnp.bfloat16)
```

```python
import functools

import jax
import jax.numpy as jnp
from jax import lax
from jax.experimental import pallas as pl
from jax.experimental.pallas import tpu as pltpu
from jax.sharding import PartitionSpec as P


def rms_norm(values, gain):
    floats = values.astype(jnp.float32)
    mean_square = jnp.mean(floats * floats, axis=-1, keepdims=True)
    return (floats * lax.rsqrt(mean_square + 1e-06) * gain).astype(jnp.bfloat16)


def routing(normed, router_weight, expert_ids):
    logits = jnp.dot(normed, router_weight, preferred_element_type=jnp.float32)
    onehot = (
        expert_ids[:, :, None] == jnp.arange(router_weight.shape[1], dtype=jnp.int32)[None, None, :]
    )
    picked = jnp.sum(jnp.where(onehot, logits[:, None, :], jnp.float32(0.0)), axis=-1)
    first_weight = jax.nn.sigmoid(picked[:, 0] - picked[:, 1])
    return jnp.stack([first_weight, 1.0 - first_weight], axis=1)


def slot_of(block_ids, experts):
    flat_ids = block_ids.reshape(-1)
    onehot = (flat_ids[:, None] == jnp.arange(experts, dtype=jnp.int32)[None, :]).astype(jnp.int32)
    before = jnp.cumsum(onehot, axis=0) - onehot
    return jnp.sum(before * onehot, axis=1).reshape(block_ids.shape)


def swiglu_hidden(inputs, gate_piece, up_piece):
    gate_part = jnp.dot(inputs, gate_piece, preferred_element_type=jnp.float32)
    up_part = jnp.dot(inputs, up_piece, preferred_element_type=jnp.float32)
    return (jax.nn.silu(gate_part) * up_part).astype(jnp.bfloat16)


def down_product(hidden, down_piece):
    return lax.dot_general(
        hidden, down_piece, (((1,), (1,)), ((), ())), preferred_element_type=jnp.float32
    )


def body(
    tokens,
    norm_gain,
    router_weight,
    shared_gate_vector,
    expert_ids,
    gate_weight,
    up_weight,
    down_weight,
    shared_gate_weight,
    shared_up_weight,
    shared_down_weight,
):
    experts = lax.axis_size("expert")
    tok_rows = tokens.shape[0]
    width = tokens.shape[1]
    capacity = 3 * tok_rows // experts
    normed = rms_norm(tokens, norm_gain)
    route_weight = routing(normed, router_weight, expert_ids)
    slot = slot_of(expert_ids, experts)
    target = expert_ids * capacity + slot
    slot_iota = jnp.arange(experts * capacity, dtype=jnp.int32)[:, None]
    dispatch_table = (
        (target[:, 0][None, :] == slot_iota) | (target[:, 1][None, :] == slot_iota)
    ).astype(jnp.bfloat16)
    outgoing = jnp.dot(dispatch_table, normed, preferred_element_type=jnp.float32).astype(
        jnp.bfloat16
    )
    outgoing = outgoing.reshape(experts, capacity, width)
    arrived = lax.all_to_all(outgoing, "expert", split_axis=0, concat_axis=0, tiled=True).reshape(
        experts * capacity, width
    )
    hidden = swiglu_hidden(
        arrived,
        lax.all_gather(gate_weight, "dp", axis=2, tiled=True)[0],
        lax.all_gather(up_weight, "dp", axis=2, tiled=True)[0],
    )
    hidden_all = hidden
    hidden = hidden_all
    expert_out = down_product(hidden, lax.all_gather(down_weight, "dp", axis=2, tiled=True)[0])
    expert_out = expert_out.astype(jnp.bfloat16).reshape(experts, capacity, width)
    returned_rows = lax.all_to_all(
        expert_out, "expert", split_axis=0, concat_axis=0, tiled=True
    ).reshape(experts * capacity, width)
    fetched = returned_rows[target].astype(jnp.float32)
    routed = jnp.sum(route_weight[:, :, None] * fetched, axis=1)
    gathered = lax.all_gather(normed, "expert", axis=0, tiled=True)
    hidden = swiglu_hidden(gathered, shared_gate_weight, shared_up_weight)
    shared = lax.psum_scatter(
        jnp.dot(hidden, shared_down_weight, preferred_element_type=jnp.float32).astype(
            jnp.bfloat16
        ),
        "expert",
        scatter_dimension=0,
        tiled=True,
    ).astype(jnp.float32)
    shared_gate = jax.nn.sigmoid(jnp.sum(normed.astype(jnp.float32) * shared_gate_vector, axis=-1))
    return (routed + shared_gate[:, None] * shared).astype(jnp.bfloat16)

MESH = pl.DeviceIdType.MESH
NONE, X, Y, XY = 0, 1, 2, 3
END, MID = 0, 1
VMEM_LIMIT = 62 * 1024 * 1024
SEMAPHORES = 192
LEAD_SHARE = 6
ANCHORS = ("S", "W", "CP", "CQ")


def operations(role):
    ops = [("S",), ("W",), ("sc", "c"), ("sc", "x"), ("sc", "y")]
    travels = [("in", 0)] if role == 0 else [("out", 1), ("in", 1), ("in", 0), ("out", 2), ("out", 3)]
    returns = [("rin", 1), ("rin", 2), ("rin", 3)] if role == 0 else [("rout", 0), ("rin", 2), ("rin", 3)]
    ops += [("sc",) + way for way in travels]
    ops += [("P",) + way + (half,) for way in travels + returns for half in range(2)]
    for plane in range(4):
        ops += [
            ("P", step, plane, half) for step in ("x", "y", "sx", "sy", "px", "py", "col") for half in range(2)
        ]
        ops += [("P", step, plane) for step in ("lo", "hi", "d", "plo", "phi")]
        ops += [(kind, *step, plane, at) for kind, *step in (("P", "c"), ("CP",), ("P", "pc")) for at in range(4)]
        ops += [(kind, *step, plane, pair) for kind, *step in (("CQ",), ("Q", "pc")) for pair in range(2)]
        ops += [("Q", "c", plane, at) for at in range(4)]
        if plane != role:
            ops += [("Q", "col", plane, at) for at in range(4)]
    ops += [("Q",) + way + (at,) for way in travels + returns for at in range(4)]
    ops += [("Q", step) for step in ("x", "y", "lo", "hi", "d", "plo", "phi", "sx", "px", "sy", "py", "end")]
    return ops


ORDER_END = (
    6, 198, 199, 49, 33, 0, 7, 2, 16, 15, 1, 200, 3, 201, 184, 55, 51, 53, 50, 183, 29, 72, 54,
    182, 52, 45, 4, 185, 67, 47, 37, 98, 41, 115, 97, 73, 68, 5, 46, 139, 48, 141, 133, 110, 111,
    75, 158, 140, 142, 176, 153, 134, 99, 118, 177, 96, 159, 154, 160, 171, 173, 175, 163, 167,
    117, 28, 56, 181, 174, 197, 180, 164, 168, 196, 143, 147, 116, 128, 161, 90, 130, 17, 170,
    172, 146, 122, 91, 126, 150, 74, 14, 36, 138, 193, 179, 131, 137, 178, 165, 169, 132, 195, 35,
    112, 113, 114, 40, 192, 44, 155, 157, 156, 34, 85, 87, 88, 194, 127, 129, 89, 30, 31, 32, 95,
    189, 94, 162, 166, 188, 136, 202, 135, 84, 191, 86, 203, 204, 144, 148, 145, 149, 79, 83, 190,
    93, 92, 121, 125, 186, 69, 70, 71, 207, 205, 120, 124, 208, 206, 187, 152, 151, 102, 103, 119,
    13, 106, 123, 100, 104, 101, 77, 12, 105, 107, 81, 78, 82, 209, 76, 80, 108, 10, 57, 61, 58,
    59, 63, 60, 39, 62, 64, 43, 109, 11, 38, 42, 20, 21, 24, 65, 8, 18, 22, 19, 23, 25, 66, 9, 26,
    27,
)
ORDER_MID = (
    12, 227, 226, 10, 104, 88, 0, 2, 13, 11, 71, 70, 1, 14, 16, 3, 228, 229, 28, 26, 106, 105,
    200, 110, 127, 45, 17, 27, 100, 15, 63, 107, 102, 92, 18, 4, 153, 109, 62, 96, 204, 145, 61,
    208, 40, 46, 41, 201, 170, 64, 19, 101, 205, 152, 103, 123, 188, 203, 212, 58, 7, 165, 209,
    154, 146, 48, 60, 50, 202, 189, 213, 54, 49, 6, 166, 122, 187, 198, 53, 57, 9, 211, 59, 30,
    151, 172, 84, 183, 199, 186, 185, 52, 210, 173, 130, 83, 29, 56, 176, 8, 196, 143, 180, 177,
    181, 171, 197, 108, 111, 144, 42, 158, 140, 142, 167, 206, 182, 168, 169, 184, 91, 47, 134,
    207, 138, 193, 225, 128, 69, 72, 129, 139, 5, 141, 192, 194, 224, 124, 175, 179, 162, 195, 43,
    157, 68, 132, 136, 217, 150, 221, 155, 161, 159, 89, 90, 156, 67, 133, 216, 137, 191, 223,
    112, 94, 160, 44, 98, 149, 220, 115, 174, 178, 119, 125, 66, 215, 190, 222, 76, 51, 55, 230,
    131, 126, 231, 34, 135, 31, 32, 33, 65, 214, 93, 232, 97, 148, 35, 219, 36, 114, 95, 99, 147,
    218, 113, 235, 73, 118, 116, 85, 233, 37, 117, 164, 25, 87, 86, 163, 24, 236, 234, 39, 21,
    120, 22, 80, 77, 74, 75, 38, 20, 121, 23, 79, 78, 237, 81, 82,
)


def flipped(position, bit):
    return position + bit - 2 * bit * ((position // bit) % 2)


def halves(count, number):
    half = count // 2 // 16 * 16
    if 2 * half == count or number in (1, 2):
        return half
    return count - half


def target(role, op):
    kind, step, rest = op[0], op[1], op[2:]
    if step in ("in", "out"):
        plane, more = rest[0], rest[1:]
        if step == "out":
            return "out", END, (kind, "z", plane) + more
        return "in", MID, (kind, "z", plane if role == END else 3 - plane) + more
    if step == "rin":
        plane, more = rest[0], rest[1:]
        if role == END:
            return "in", MID, (kind, "rz", 1, plane) + more
        return "in", MID, (kind, "rz", 0, 3 - plane) + more
    if step == "rout":
        return "out", END, (kind, "rz", 0) + rest
    if step in ("c", "pc"):
        return "c", role, op
    return ("x" if step in ("x", "lo", "plo", "px") else "y"), role, op


def fused_kernel(
    rows,
    lead,
    hidden_units,
    shared_units,
    tokens_ref,
    gain_ref,
    router_ref,
    vector_ref,
    ids_ref,
    gate_ref,
    up_ref,
    down_ref,
    sgate_ref,
    sup_ref,
    sdown_ref,
    out_ref,
    sc,
    tok_p,
    tok_q,
    part_p,
    part_q,
    core_p,
    core_q,
    diag_p,
    diag_q,
    x_p,
    x_q,
    y_p,
    y_q,
    line_p,
    line_q,
    w_gate,
    w_up,
    down_raw,
    w_down,
    send_sem,
    recv_sem,
    load_sem,
):
    e_at = lax.axis_index("expert")
    d_at = lax.axis_index("dp")
    rest = rows - lead
    z_at = d_at // 2
    toward = 2 * (1 - 2 * (z_at // 2))
    mid = (z_at + z_at // 2) % 2
    partner = {
        "c": (flipped(e_at, 1), d_at),
        "x": (flipped(e_at, 2), d_at),
        "y": (e_at, flipped(d_at, 1)),
        "in": (e_at, d_at + toward),
        "out": (e_at, d_at - toward),
    }
    barrier = pltpu.get_barrier_semaphore()
    for to in ("c", "x", "y", "in"):
        pl.semaphore_signal(barrier, inc=1, device_id=partner[to], device_id_type=MESH)

    @pl.when(mid == 1)
    def _():
        pl.semaphore_signal(barrier, inc=1, device_id=partner["out"], device_id_type=MESH)

    first = pl.multiple_of(d_at * shared_units, shared_units)
    loads = [
        pltpu.make_async_copy(gate_ref.at[0], w_gate.at[:, pl.ds(0, hidden_units)], load_sem.at[0]),
        pltpu.make_async_copy(up_ref.at[0], w_up.at[:, pl.ds(0, hidden_units)], load_sem.at[1]),
        pltpu.make_async_copy(
            sgate_ref.at[:, pl.ds(first, shared_units)],
            w_gate.at[:, pl.ds(hidden_units, shared_units)],
            load_sem.at[2],
        ),
        pltpu.make_async_copy(
            sup_ref.at[:, pl.ds(first, shared_units)],
            w_up.at[:, pl.ds(hidden_units, shared_units)],
            load_sem.at[3],
        ),
        pltpu.make_async_copy(
            sdown_ref.at[pl.ds(first, shared_units), :],
            w_down.at[pl.ds(hidden_units, shared_units), :],
            load_sem.at[4],
        ),
        pltpu.make_async_copy(down_ref.at[0], down_raw, load_sem.at[5]),
    ]
    for load in loads:
        load.start()

    floats = tokens_ref[...].astype(jnp.float32)
    mean_square = jnp.mean(floats * floats, axis=-1, keepdims=True)
    normed = (floats * lax.rsqrt(mean_square + 1e-06) * gain_ref[...][None, :]).astype(jnp.bfloat16)
    tok_p[mid, NONE, 0] = normed[:lead]
    tok_q[mid, NONE, 0] = normed[lead:]
    pl.semaphore_wait(barrier, 4 + mid)

    lines = sc.shape[3]
    def make_scales():
        normed = jnp.concatenate([tok_p[mid, NONE, 0], tok_q[mid, NONE, 0]], axis=0)
        logits = lax.dot_general(
            router_ref[...], normed, (((1,), (1,)), ((), ())), preferred_element_type=jnp.float32
        )
        ids = ids_ref[...]
        first_id, second_id = ids[0:1], ids[1:2]
        row = lax.broadcasted_iota(jnp.int32, logits.shape, 0)
        margin = jnp.sum(
            jnp.where(row == first_id, logits, 0.0), axis=0, keepdims=True
        ) - jnp.sum(jnp.where(row == second_id, logits, 0.0), axis=0, keepdims=True)
        first_weight = jax.nn.sigmoid(margin)
        shared_gate = jax.nn.sigmoid(
            jnp.sum(normed.astype(jnp.float32) * vector_ref[...][None, :], axis=-1, keepdims=True)
        )
        column = lax.broadcasted_iota(jnp.int32, (rows, lines), 1)
        row = lax.broadcasted_iota(jnp.int32, (lines, rows), 0)
        scales = jnp.transpose(jnp.where(column == lines - 1, shared_gate, 0.0))
        scales = scales + jnp.where(row == first_id, first_weight, 0.0)
        scales = scales + jnp.where(row == second_id, 1.0 - first_weight, 0.0)
        sc[mid, NONE, 0] = scales

    numbers = {}

    def number(name):
        return numbers.setdefault(name, len(numbers))

    def landing(role, name):
        kind, step = name[0], name[1]
        if kind == "sc":
            if step == "z":
                return sc.at[name[2]]
            return {"c": sc.at[role, NONE, 1], "x": sc.at[role, X], "y": sc.at[role, pl.ds(2, 2)]}[step]
        if kind == "P":
            plane = name[3] if step == "rz" else name[2]
            at = halves(lead, plane)
            low, high = pl.ds(0, at), pl.ds(at, lead - at)
            if step == "rz":
                return line_p.at[name[2], plane, high if name[4] else low]
            if step == "c":
                return tok_p.at[plane, name[3], 1]
            if step == "pc":
                return core_p.at[plane, name[3]]
            if step in ("z", "x", "y"):
                place = {"z": NONE, "x": X, "y": Y}[step]
                return tok_p.at[plane, place, 0, high if name[3] else low]
            if step in ("px", "py"):
                return (x_p if step == "px" else y_p).at[plane, high if name[3] else low]
            return {
                "lo": tok_p.at[plane, XY, 0, low],
                "hi": tok_p.at[plane, XY, 0, high],
                "plo": diag_p.at[plane, low],
                "phi": diag_p.at[plane, high],
            }[step]
        at = halves(rest, role)
        low, high = pl.ds(0, at), pl.ds(at, rest - at)
        if step == "rz":
            return line_q.at[name[2], name[3], name[4]]
        if step == "z":
            return tok_q.at[name[2], name[3], 0]
        if step == "c":
            return tok_q.at[name[2], name[3], 1]
        if step == "pc":
            return core_q.at[name[2], pl.ds(2 * name[3], 2)]
        return {
            "x": tok_q.at[role, X, 0],
            "y": tok_q.at[role, Y, 0],
            "lo": tok_q.at[role, XY, 0, low],
            "hi": tok_q.at[role, XY, 0, high],
            "plo": diag_q.at[low],
            "phi": diag_q.at[high],
            "px": x_q,
            "py": y_q,
        }[step]

    def source(role, op):
        kind, step = op[0], op[1]
        if kind == "sc":
            if step in ("in", "out"):
                return sc.at[op[2]]
            return {"c": sc.at[role, NONE, 0], "x": sc.at[role, NONE], "y": sc.at[role, pl.ds(0, 2)]}[
                step
            ]
        if kind == "P":
            plane = op[2]
            at = halves(lead, plane)
            low, high = pl.ds(0, at), pl.ds(at, lead - at)
            if step == "c":
                return tok_p.at[plane, op[3], 0]
            if step == "pc":
                return part_p.at[plane, op[3], 1]
            if step in ("in", "out", "x", "y"):
                return tok_p.at[plane, NONE, 0, high if op[3] else low]
            if step in ("px", "py", "rin", "rout"):
                place = {"px": X, "py": Y}.get(step, NONE)
                return part_p.at[plane, place, 0, high if op[3] else low]
            return {
                "lo": tok_p.at[plane, Y, 0, low],
                "hi": tok_p.at[plane, X, 0, high],
                "plo": part_p.at[plane, XY, 0, low],
                "phi": part_p.at[plane, XY, 0, high],
            }[step]
        at = halves(rest, role)
        low, high = pl.ds(0, at), pl.ds(at, rest - at)
        if step in ("in", "out", "c"):
            return tok_q.at[op[2], op[3], 0]
        if step == "pc":
            return part_q.at[op[2], pl.ds(2 * op[3], 2), 1]
        if step in ("rin", "rout"):
            return part_q.at[op[2], op[3], 0]
        return {
            "x": tok_q.at[role, NONE, 0],
            "y": tok_q.at[role, NONE, 0],
            "lo": tok_q.at[role, Y, 0, low],
            "hi": tok_q.at[role, X, 0, high],
            "plo": part_q.at[role, XY, 0, low],
            "phi": part_q.at[role, XY, 0, high],
            "px": part_q.at[role, X, 0],
            "py": part_q.at[role, Y, 0],
        }[step]

    arrived = set()
    sent = {END: [], MID: []}

    def arrive(role, *names):
        for name in names:
            if (role, name) in arrived:
                continue
            arrived.add((role, name))
            ref = landing(role, name)
            pltpu.make_async_remote_copy(
                src_ref=ref,
                dst_ref=ref,
                send_sem=send_sem.at[0],
                recv_sem=recv_sem.at[number(name)],
                device_id=partner["c"],
                device_id_type=MESH,
            ).wait_recv()

    def block_here(role, kind, plane, at):
        if kind == "Q":
            if plane != role:
                return [("Q", "z", plane, at)]
            return {
                NONE: [],
                X: [("Q", "x")],
                Y: [("Q", "y")],
                XY: [("Q", "lo"), ("Q", "hi")],
            }[at]
        if at == XY:
            return [("P", "lo", plane), ("P", "hi", plane)]
        if at == NONE and plane == role:
            return []
        return [("P", ("z", "x", "y")[at], plane, part) for part in range(2)]

    def scales_here(role, plane, at):
        if plane != role:
            return [("sc", "z", plane)]
        return [[("sc", "c")], [("sc", "x")], [("sc", "y")], [("sc", "y")]][at]

    def needs(role, op):
        kind, step = op[0], op[1]
        if kind == "sc":
            if step in ("in", "out"):
                return scales_here(role, op[2], XY)
            return {"c": [], "x": [("sc", "c")], "y": [("sc", "x")]}[step]
        if step == "c":
            return block_here(role, kind, op[2], op[3])
        if step == "lo":
            return [("P", "y", op[2], 0)] if kind == "P" else [("Q", "y")]
        if step == "hi":
            return [("P", "x", op[2], 1)] if kind == "P" else [("Q", "x")]
        if step in ("in", "out", "x", "y"):
            if kind == "P":
                return [] if op[2] == role else [("P", "z", op[2], op[3])]
            return block_here(role, kind, op[2], op[3]) if step in ("in", "out") else []
        return []

    def copy_of(role, op, at):
        link, _, name = target(role, op)
        there = END if link == "out" else MID if link == "in" else role
        return pltpu.make_async_remote_copy(
            src_ref=source(role, op),
            dst_ref=landing(there, name),
            send_sem=send_sem.at[at],
            recv_sem=recv_sem.at[number(name)],
            device_id=partner[link],
            device_id_type=MESH,
        )

    def send(role, op):
        arrive(role, *needs(role, op))
        copy_of(role, op, len(sent[role])).start()
        sent[role].append(op)

    def f32(values):
        return values.astype(jnp.float32)

    def sides(role, plane):
        if role == plane:
            return (0,) if role == END else (1, 0)
        if role == END:
            return ()
        return (0,) if plane == END else (1,)

    def bf16(values):
        return values.astype(jnp.bfloat16)

    def chip_p(role, plane, at, span):
        arrive(role, ("P", "pc", plane, at))
        return f32(part_p[plane, at, 0, span]) + f32(core_p[plane, at, span])

    def chip_q(role, plane, at):
        arrive(role, ("Q", "pc", plane, at // 2))
        total = f32(part_q[plane, at, 0]) + f32(core_q[plane, at])
        for side in sides(role, plane):
            arrive(role, ("Q", "rz", side, plane, at))
            total = total + f32(line_q[side, plane, at])
        return total

    def add_p(role, step, plane, part=None):
        cut = halves(lead, plane)
        span = slice(cut, lead) if part else slice(0, cut)
        if step == "d":
            part_p[plane, XY, 0] = bf16(chip_p(role, plane, XY, slice(0, lead)))
        elif step in ("sx", "sy"):
            at = X if step == "sx" else Y
            total = chip_p(role, plane, at, span)
            if part == (1 if step == "sx" else 0):
                arrive(role, ("P", "phi" if step == "sx" else "plo", plane))
                total = total + f32(diag_p[plane, span])
            part_p[plane, at, 0, span] = bf16(total)
        else:
            total = chip_p(role, plane, NONE, span)
            arrive(role, ("P", "px", plane, part), ("P", "py", plane, part))
            total = total + f32(x_p[plane, span]) + f32(y_p[plane, span])
            for side in sides(role, plane):
                arrive(role, ("P", "rz", side, plane, part))
                total = total + f32(line_p[side, plane, span])
            if plane == role:
                out_ref[span] = total.astype(out_ref.dtype)
            else:
                part_p[plane, NONE, 0, span] = bf16(total)

    def add_q(role, step, *more):
        cut = halves(rest, role)
        if step == "col":
            plane, at = more
            part_q[plane, at, 0] = bf16(chip_q(role, plane, at))
        elif step == "d":
            part_q[role, XY, 0] = bf16(chip_q(role, role, XY))
        elif step == "sx":
            total = chip_q(role, role, X)
            arrive(role, ("Q", "phi"))
            part_q[role, X, 0, :cut] = bf16(total[:cut])
            part_q[role, X, 0, cut:] = bf16(total[cut:] + f32(diag_q[cut:]))
        elif step == "sy":
            total = chip_q(role, role, Y)
            arrive(role, ("Q", "plo"))
            part_q[role, Y, 0, :cut] = bf16(total[:cut] + f32(diag_q[:cut]))
            part_q[role, Y, 0, cut:] = bf16(total[cut:])
        else:
            total = chip_q(role, role, NONE)
            arrive(role, ("Q", "px"), ("Q", "py"))
            out_ref[lead:] = (total + f32(x_q[...]) + f32(y_q[...])).astype(out_ref.dtype)

    def scale_columns(blocks, low, high):
        line = lax.broadcasted_iota(jnp.int32, (high - low, lines), 1)
        routed, shared = [], []
        for block in blocks:
            columns = jnp.transpose(block)[low:high]
            routed.append(jnp.sum(jnp.where(line == e_at, columns, 0.0), axis=1, keepdims=True))
            shared.append(columns[:, lines - 1 :])
        return jnp.concatenate(routed, axis=0), jnp.concatenate(shared, axis=0)

    def experts(inputs, scales):
        routed_scale, shared_scale = scales
        gate_part = jnp.dot(inputs, w_gate[...], preferred_element_type=jnp.float32)
        up_part = jnp.dot(inputs, w_up[...], preferred_element_type=jnp.float32)
        hidden = gate_part * jax.nn.sigmoid(gate_part) * up_part
        hidden = jnp.concatenate(
            [
                bf16(hidden[:, :hidden_units] * routed_scale),
                bf16(hidden[:, hidden_units:] * shared_scale),
            ],
            axis=1,
        )
        return bf16(jnp.dot(hidden, w_down[...], preferred_element_type=jnp.float32))

    def by_role(at_end, at_mid):
        return at_end if at_end == at_mid else at_end + (at_mid - at_end) * mid

    def compute(op_end, op_mid):
        plane, at = by_role(op_end[1], op_mid[1]), by_role(op_end[2], op_mid[2])
        width = tok_p.shape[4]
        if op_end[0] == "CP":
            inputs = tok_p[plane, at].reshape(2 * lead, width)
            blocks = [sc[plane, at, core] for core in range(2)]
            result = experts(inputs, scale_columns(blocks, 0, lead))
            part_p[plane, at] = result.reshape(2, lead, width)
        else:
            pair = pl.ds(2 * at, 2)
            inputs = tok_q[plane, pair].reshape(4 * rest, width)
            blocks = [sc[plane, 2 * at + one, core] for one in range(2) for core in range(2)]
            result = experts(inputs, scale_columns(blocks, lead, rows))
            part_q[plane, pair] = result.reshape(2, 2, rest, width)

    def ready(role, op):
        plane, at = op[1], op[2]
        if op[0] == "CP":
            arrive(role, *block_here(role, "P", plane, at), ("P", "c", plane, at))
            arrive(role, *scales_here(role, plane, at))
        else:
            for one in (2 * at, 2 * at + 1):
                arrive(role, *block_here(role, "Q", plane, one), ("Q", "c", plane, one))
                arrive(role, *scales_here(role, plane, one))

    def anchors(role, order):
        parts, ops = [[]], operations(role)
        for op in (ops[at] for at in order):
            parts[-1].append(op)
            if op[0] in ANCHORS:
                parts.append([])
        return parts

    def run(role, part):
        for op in part:
            if op[0] in ("S", "W"):
                continue
            if op[0] in ("CP", "CQ"):
                ready(role, op)
            elif op[0] == "P" and op[1] in ("d", "sx", "sy", "col"):
                add_p(role, *op[1:])
            elif op[0] == "Q" and op[1] in ("d", "sx", "sy", "col", "end"):
                add_q(role, *op[1:])
            else:
                send(role, op)

    for part_end, part_mid in zip(anchors(END, ORDER_END), anchors(MID, ORDER_MID), strict=True):

        @pl.when(mid == 0)
        def _():
            run(END, part_end)

        @pl.when(mid == 1)
        def _():
            run(MID, part_mid)

        if not part_end or part_end[-1][0] not in ANCHORS:
            continue
        if part_end[-1][0] == "S":
            make_scales()
        elif part_end[-1][0] == "W":
            for load in loads:
                load.wait()
            w_down[0:hidden_units, :] = jnp.transpose(down_raw[...])
        else:
            compute(part_end[-1], part_mid[-1])

    @pl.when(mid == 0)
    def _():
        for at, op in enumerate(sent[END]):
            copy_of(END, op, at).wait_send()

    @pl.when(mid == 1)
    def _():
        for at, op in enumerate(sent[MID]):
            copy_of(MID, op, at).wait_send()


def fused_body(
    tokens,
    norm_gain,
    router_weight,
    shared_gate_vector,
    expert_ids,
    gate_weight,
    up_weight,
    down_weight,
    shared_gate_weight,
    shared_up_weight,
    shared_down_weight,
):
    rows, width = tokens.shape
    hidden_units = gate_weight.shape[2]
    shared_units = shared_gate_weight.shape[1] // lax.axis_size("dp")
    units = hidden_units + shared_units
    lead = LEAD_SHARE * rows // 8
    rest = rows - lead
    anywhere = pl.BlockSpec(memory_space=pl.ANY)

    def blocks(count, *planes):
        return pltpu.VMEM(planes + (count, width), jnp.bfloat16)

    return pl.pallas_call(
        functools.partial(fused_kernel, rows, lead, hidden_units, shared_units),
        out_shape=jax.ShapeDtypeStruct((rows, width), jnp.bfloat16),
        in_specs=[pl.BlockSpec(memory_space=pltpu.VMEM)] * 5 + [anywhere] * 6,
        out_specs=pl.BlockSpec(memory_space=pltpu.VMEM),
        scratch_shapes=[
            pltpu.VMEM((4, 4, 2, 8, rows), jnp.float32),
            blocks(lead, 4, 4, 2),
            blocks(rest, 4, 4, 2),
            blocks(lead, 4, 4, 2),
            blocks(rest, 4, 4, 2),
            blocks(lead, 4, 4),
            blocks(rest, 4, 4),
            blocks(lead, 4),
            blocks(rest),
            blocks(lead, 4),
            blocks(rest),
            blocks(lead, 4),
            blocks(rest),
            blocks(lead, 2, 4),
            blocks(rest, 2, 4, 4),
            pltpu.VMEM((width, units), jnp.bfloat16),
            pltpu.VMEM((width, units), jnp.bfloat16),
            pltpu.VMEM((width, hidden_units), jnp.bfloat16),
            pltpu.VMEM((units, width), jnp.bfloat16),
            pltpu.SemaphoreType.DMA((SEMAPHORES,)),
            pltpu.SemaphoreType.DMA((SEMAPHORES,)),
            pltpu.SemaphoreType.DMA((6,)),
        ],
        compiler_params=pltpu.CompilerParams(
            collective_id=0, has_side_effects=True, vmem_limit_bytes=VMEM_LIMIT
        ),
    )(
        tokens,
        norm_gain,
        router_weight.T,
        shared_gate_vector,
        expert_ids.T,
        gate_weight,
        up_weight,
        down_weight,
        shared_gate_weight,
        shared_up_weight,
        shared_down_weight,
    )


def solution(mesh):
    fused = (mesh.shape["expert"], mesh.shape["dp"]) == (1 << 2, 1 << 3)
    return jax.shard_map(
        fused_body if fused else body,
        mesh=mesh,
        in_specs=(
            P(("expert", "dp"), None),
            P(),
            P(),
            P(),
            P(("expert", "dp"), None),
            P("expert", None, "dp"),
            P("expert", None, "dp"),
            P("expert", None, "dp"),
            P(None, "expert"),
            P(None, "expert"),
            P("expert", None),
        ),
        out_specs=P(("expert", "dp"), None),
        check_vma=False,
    )
```

```python
import functools

import jax
import jax.numpy as jnp
from jax import lax
from jax.experimental import pallas as pl
from jax.experimental.pallas import tpu as pltpu
from jax.sharding import PartitionSpec as P


def rms_norm(values, gain):
    floats = values.astype(jnp.float32)
    mean_square = jnp.mean(floats * floats, axis=-1, keepdims=True)
    return (floats * lax.rsqrt(mean_square + 1e-06) * gain).astype(jnp.bfloat16)


def routing(normed, router_weight, expert_ids):
    logits = jnp.dot(normed, router_weight, preferred_element_type=jnp.float32)
    onehot = (
        expert_ids[:, :, None] == jnp.arange(router_weight.shape[1], dtype=jnp.int32)[None, None, :]
    )
    picked = jnp.sum(jnp.where(onehot, logits[:, None, :], jnp.float32(0.0)), axis=-1)
    first_weight = jax.nn.sigmoid(picked[:, 0] - picked[:, 1])
    return jnp.stack([first_weight, 1.0 - first_weight], axis=1)


def slot_of(block_ids, experts):
    flat_ids = block_ids.reshape(-1)
    onehot = (flat_ids[:, None] == jnp.arange(experts, dtype=jnp.int32)[None, :]).astype(jnp.int32)
    before = jnp.cumsum(onehot, axis=0) - onehot
    return jnp.sum(before * onehot, axis=1).reshape(block_ids.shape)


def swiglu_hidden(inputs, gate_piece, up_piece):
    gate_part = jnp.dot(inputs, gate_piece, preferred_element_type=jnp.float32)
    up_part = jnp.dot(inputs, up_piece, preferred_element_type=jnp.float32)
    return (jax.nn.silu(gate_part) * up_part).astype(jnp.bfloat16)


def down_product(hidden, down_piece):
    return lax.dot_general(
        hidden, down_piece, (((1,), (1,)), ((), ())), preferred_element_type=jnp.float32
    )


def body(
    tokens,
    norm_gain,
    router_weight,
    shared_gate_vector,
    expert_ids,
    gate_weight,
    up_weight,
    down_weight,
    shared_gate_weight,
    shared_up_weight,
    shared_down_weight,
):
    experts = lax.axis_size("expert")
    tok_rows = tokens.shape[0]
    width = tokens.shape[1]
    capacity = 3 * tok_rows // experts
    normed = rms_norm(tokens, norm_gain)
    route_weight = routing(normed, router_weight, expert_ids)
    slot = slot_of(expert_ids, experts)
    target = expert_ids * capacity + slot
    slot_iota = jnp.arange(experts * capacity, dtype=jnp.int32)[:, None]
    dispatch_table = (
        (target[:, 0][None, :] == slot_iota) | (target[:, 1][None, :] == slot_iota)
    ).astype(jnp.bfloat16)
    outgoing = jnp.dot(dispatch_table, normed, preferred_element_type=jnp.float32).astype(
        jnp.bfloat16
    )
    outgoing = outgoing.reshape(experts, capacity, width)
    arrived = lax.all_to_all(outgoing, "expert", split_axis=0, concat_axis=0, tiled=True).reshape(
        experts * capacity, width
    )
    hidden = swiglu_hidden(
        arrived,
        lax.all_gather(gate_weight, "dp", axis=2, tiled=True)[0],
        lax.all_gather(up_weight, "dp", axis=2, tiled=True)[0],
    )
    hidden_all = hidden
    hidden = hidden_all
    expert_out = down_product(hidden, lax.all_gather(down_weight, "dp", axis=2, tiled=True)[0])
    expert_out = expert_out.astype(jnp.bfloat16).reshape(experts, capacity, width)
    returned_rows = lax.all_to_all(
        expert_out, "expert", split_axis=0, concat_axis=0, tiled=True
    ).reshape(experts * capacity, width)
    fetched = returned_rows[target].astype(jnp.float32)
    routed = jnp.sum(route_weight[:, :, None] * fetched, axis=1)
    gathered = lax.all_gather(normed, "expert", axis=0, tiled=True)
    hidden = swiglu_hidden(gathered, shared_gate_weight, shared_up_weight)
    shared = lax.psum_scatter(
        jnp.dot(hidden, shared_down_weight, preferred_element_type=jnp.float32).astype(
            jnp.bfloat16
        ),
        "expert",
        scatter_dimension=0,
        tiled=True,
    ).astype(jnp.float32)
    shared_gate = jax.nn.sigmoid(jnp.sum(normed.astype(jnp.float32) * shared_gate_vector, axis=-1))
    return (routed + shared_gate[:, None] * shared).astype(jnp.bfloat16)

MESH = pl.DeviceIdType.MESH
NONE, X, Y, XY = 0, 1, 2, 3
END, MID = 0, 1
VMEM_LIMIT = 62 * 1024 * 1024
SEMAPHORES = 192
LEAD_SHARE = 6
ANCHORS = ("S", "W", "CP", "CQ")


def operations(role):
    ops = [("S",), ("W",), ("sc", "c"), ("sc", "x"), ("sc", "y")]
    travels = [("in", 0)] if role == 0 else [("out", 1), ("in", 1), ("in", 0), ("out", 2), ("out", 3)]
    returns = [("rin", 1), ("rin", 2), ("rin", 3)] if role == 0 else [("rout", 0), ("rin", 2), ("rin", 3)]
    ops += [("sc",) + way for way in travels]
    ops += [("P",) + way + (half,) for way in travels + returns for half in range(2)]
    for plane in range(4):
        ops += [
            ("P", step, plane, half) for step in ("x", "y", "sx", "sy", "px", "py", "col") for half in range(2)
        ]
        ops += [("P", step, plane) for step in ("lo", "hi", "d", "plo", "phi")]
        ops += [(kind, *step, plane, at) for kind, *step in (("P", "c"), ("CP",), ("P", "pc")) for at in range(4)]
        ops += [(kind, *step, plane, pair) for kind, *step in (("CQ",), ("Q", "pc")) for pair in range(2)]
        ops += [("Q", "c", plane, at) for at in range(4)]
        if plane != role:
            ops += [("Q", "col", plane, at) for at in range(4)]
    ops += [("Q",) + way + (at,) for way in travels + returns for at in range(4)]
    ops += [("Q", step) for step in ("x", "y", "lo", "hi", "d", "plo", "phi", "sx", "px", "sy", "py", "end")]
    return ops


ORDER_END = (
    6, 198, 199, 49, 33, 0, 7, 2, 15, 17, 1, 200, 201, 3, 184, 55, 51, 53, 50, 37, 41, 182, 29,
    72, 54, 183, 52, 45, 185, 4, 96, 47, 98, 115, 97, 73, 99, 5, 46, 139, 48, 141, 133, 110, 116,
    111, 117, 158, 140, 142, 176, 134, 153, 68, 118, 177, 67, 159, 154, 160, 171, 173, 174, 163,
    167, 14, 16, 181, 197, 180, 128, 130, 131, 196, 122, 161, 90, 126, 75, 56, 138, 193, 143, 147,
    137, 164, 175, 28, 168, 192, 35, 34, 112, 114, 165, 169, 91, 146, 121, 113, 150, 125, 74, 132,
    155, 170, 172, 79, 156, 157, 88, 83, 36, 179, 195, 178, 103, 85, 87, 89, 194, 107, 102, 69,
    70, 127, 129, 202, 95, 189, 94, 120, 124, 71, 188, 203, 144, 148, 136, 135, 145, 162, 149,
    191, 166, 100, 101, 105, 119, 190, 123, 207, 208, 40, 44, 104, 152, 13, 77, 106, 81, 151, 12,
    30, 31, 109, 78, 204, 82, 58, 32, 57, 84, 86, 61, 11, 76, 80, 59, 63, 93, 187, 108, 92, 62,
    60, 205, 39, 10, 43, 64, 38, 206, 42, 20, 21, 186, 25, 65, 18, 22, 19, 8, 23, 24, 209, 66, 9,
    27, 26,
)
ORDER_MID = (
    12, 227, 10, 226, 104, 88, 0, 13, 2, 11, 70, 71, 1, 14, 3, 16, 229, 228, 110, 26, 106, 105,
    92, 96, 200, 28, 45, 17, 127, 27, 100, 15, 107, 63, 102, 4, 18, 109, 153, 61, 204, 145, 208,
    62, 122, 46, 41, 201, 170, 19, 64, 101, 205, 103, 152, 123, 188, 202, 212, 58, 7, 165, 209,
    146, 111, 60, 49, 6, 198, 213, 189, 53, 57, 166, 40, 186, 130, 59, 50, 9, 210, 199, 54, 83,
    174, 203, 29, 129, 8, 143, 178, 30, 134, 206, 173, 154, 48, 108, 144, 138, 133, 196, 137, 183,
    187, 211, 185, 84, 151, 47, 124, 177, 197, 181, 115, 128, 69, 140, 126, 172, 142, 182, 207,
    184, 193, 225, 167, 168, 171, 169, 91, 52, 5, 194, 56, 192, 224, 176, 195, 180, 72, 125, 89,
    150, 221, 68, 42, 149, 175, 217, 44, 179, 43, 220, 158, 157, 67, 95, 99, 216, 156, 160, 155,
    114, 162, 90, 51, 55, 85, 132, 136, 159, 161, 191, 223, 32, 31, 33, 190, 222, 139, 141, 34,
    112, 36, 113, 94, 98, 230, 66, 215, 131, 231, 119, 116, 135, 65, 214, 76, 148, 219, 93, 118,
    97, 147, 218, 117, 235, 73, 236, 164, 86, 25, 37, 163, 24, 77, 87, 121, 23, 35, 75, 232, 38,
    20, 80, 74, 78, 120, 22, 79, 39, 21, 233, 234, 237, 81, 82,
)


def flipped(position, bit):
    return position + bit - 2 * bit * ((position // bit) % 2)


def halves(count, number):
    half = count // 2 // 16 * 16
    if 2 * half == count or number in (1, 2):
        return half
    return count - half


def target(role, op):
    kind, step, rest = op[0], op[1], op[2:]
    if step in ("in", "out"):
        plane, more = rest[0], rest[1:]
        if step == "out":
            return "out", END, (kind, "z", plane) + more
        return "in", MID, (kind, "z", plane if role == END else 3 - plane) + more
    if step == "rin":
        plane, more = rest[0], rest[1:]
        if role == END:
            return "in", MID, (kind, "rz", 1, plane) + more
        return "in", MID, (kind, "rz", 0, 3 - plane) + more
    if step == "rout":
        return "out", END, (kind, "rz", 0) + rest
    if step in ("c", "pc"):
        return "c", role, op
    return ("x" if step in ("x", "lo", "plo", "px") else "y"), role, op


def fused_kernel(
    rows,
    lead,
    hidden_units,
    shared_units,
    tokens_in,
    gain_in,
    router_in,
    vector_in,
    ids_in,
    gate_ref,
    up_ref,
    down_ref,
    sgate_ref,
    sup_ref,
    sdown_ref,
    out_ref,
    tokens_ref,
    gain_ref,
    router_ref,
    vector_ref,
    ids_ref,
    sc,
    tok_p,
    tok_q,
    part_p,
    part_q,
    core_p,
    core_q,
    diag_p,
    diag_q,
    x_p,
    x_q,
    y_p,
    y_q,
    line_p,
    line_q,
    w_gate,
    w_up,
    down_raw,
    w_down,
    send_sem,
    recv_sem,
    load_sem,
):
    e_at = lax.axis_index("expert")
    d_at = lax.axis_index("dp")
    rest = rows - lead
    z_at = d_at // 2
    toward = 2 * (1 - 2 * (z_at // 2))
    mid = (z_at + z_at // 2) % 2
    partner = {
        "c": (flipped(e_at, 1), d_at),
        "x": (flipped(e_at, 2), d_at),
        "y": (e_at, flipped(d_at, 1)),
        "in": (e_at, d_at + toward),
        "out": (e_at, d_at - toward),
    }
    barrier = pltpu.get_barrier_semaphore()
    for to in ("c", "x", "y", "in"):
        pl.semaphore_signal(barrier, inc=1, device_id=partner[to], device_id_type=MESH)

    @pl.when(mid == 1)
    def _():
        pl.semaphore_signal(barrier, inc=1, device_id=partner["out"], device_id_type=MESH)

    inputs = [
        pltpu.make_async_copy(there, here, load_sem.at[6 + at])
        for at, (there, here) in enumerate(
            (
                (tokens_in, tokens_ref),
                (gain_in, gain_ref),
                (router_in, router_ref),
                (vector_in, vector_ref),
                (ids_in, ids_ref),
            )
        )
    ]
    for load in inputs:
        load.start()

    first = pl.multiple_of(d_at * shared_units, shared_units)
    loads = [
        pltpu.make_async_copy(gate_ref.at[0], w_gate.at[:, pl.ds(0, hidden_units)], load_sem.at[0]),
        pltpu.make_async_copy(up_ref.at[0], w_up.at[:, pl.ds(0, hidden_units)], load_sem.at[1]),
        pltpu.make_async_copy(
            sgate_ref.at[:, pl.ds(first, shared_units)],
            w_gate.at[:, pl.ds(hidden_units, shared_units)],
            load_sem.at[2],
        ),
        pltpu.make_async_copy(
            sup_ref.at[:, pl.ds(first, shared_units)],
            w_up.at[:, pl.ds(hidden_units, shared_units)],
            load_sem.at[3],
        ),
        pltpu.make_async_copy(
            sdown_ref.at[pl.ds(first, shared_units), :],
            w_down.at[pl.ds(hidden_units, shared_units), :],
            load_sem.at[4],
        ),
        pltpu.make_async_copy(down_ref.at[0], down_raw, load_sem.at[5]),
    ]
    for load in loads:
        load.start()
    for load in inputs:
        load.wait()

    floats = tokens_ref[...].astype(jnp.float32)
    mean_square = jnp.mean(floats * floats, axis=-1, keepdims=True)
    normed = (floats * lax.rsqrt(mean_square + 1e-06) * gain_ref[...][None, :]).astype(jnp.bfloat16)
    tok_p[mid, NONE, 0] = normed[:lead]
    tok_q[mid, NONE, 0] = normed[lead:]
    pl.semaphore_wait(barrier, 4 + mid)

    lines = sc.shape[3]
    def make_scales():
        normed = jnp.concatenate([tok_p[mid, NONE, 0], tok_q[mid, NONE, 0]], axis=0)
        logits = lax.dot_general(
            router_ref[...], normed, (((1,), (1,)), ((), ())), preferred_element_type=jnp.float32
        )
        ids = ids_ref[...]
        first_id, second_id = ids[0:1], ids[1:2]
        row = lax.broadcasted_iota(jnp.int32, logits.shape, 0)
        margin = jnp.sum(
            jnp.where(row == first_id, logits, 0.0), axis=0, keepdims=True
        ) - jnp.sum(jnp.where(row == second_id, logits, 0.0), axis=0, keepdims=True)
        first_weight = jax.nn.sigmoid(margin)
        shared_gate = jax.nn.sigmoid(
            jnp.sum(normed.astype(jnp.float32) * vector_ref[...][None, :], axis=-1, keepdims=True)
        )
        column = lax.broadcasted_iota(jnp.int32, (rows, lines), 1)
        row = lax.broadcasted_iota(jnp.int32, (lines, rows), 0)
        scales = jnp.transpose(jnp.where(column == lines - 1, shared_gate, 0.0))
        scales = scales + jnp.where(row == first_id, first_weight, 0.0)
        scales = scales + jnp.where(row == second_id, 1.0 - first_weight, 0.0)
        sc[mid, NONE, 0] = scales

    numbers = {}

    def number(name):
        return numbers.setdefault(name, len(numbers))

    def landing(role, name):
        kind, step = name[0], name[1]
        if kind == "sc":
            if step == "z":
                return sc.at[name[2]]
            return {"c": sc.at[role, NONE, 1], "x": sc.at[role, X], "y": sc.at[role, pl.ds(2, 2)]}[step]
        if kind == "P":
            plane = name[3] if step == "rz" else name[2]
            at = halves(lead, plane)
            low, high = pl.ds(0, at), pl.ds(at, lead - at)
            if step == "rz":
                return line_p.at[name[2], plane, high if name[4] else low]
            if step == "c":
                return tok_p.at[plane, name[3], 1]
            if step == "pc":
                return core_p.at[plane, name[3]]
            if step in ("z", "x", "y"):
                place = {"z": NONE, "x": X, "y": Y}[step]
                return tok_p.at[plane, place, 0, high if name[3] else low]
            if step in ("px", "py"):
                return (x_p if step == "px" else y_p).at[plane, high if name[3] else low]
            return {
                "lo": tok_p.at[plane, XY, 0, low],
                "hi": tok_p.at[plane, XY, 0, high],
                "plo": diag_p.at[plane, low],
                "phi": diag_p.at[plane, high],
            }[step]
        at = halves(rest, role)
        low, high = pl.ds(0, at), pl.ds(at, rest - at)
        if step == "rz":
            return line_q.at[name[2], name[3], name[4]]
        if step == "z":
            return tok_q.at[name[2], name[3], 0]
        if step == "c":
            return tok_q.at[name[2], name[3], 1]
        if step == "pc":
            return core_q.at[name[2], pl.ds(2 * name[3], 2)]
        return {
            "x": tok_q.at[role, X, 0],
            "y": tok_q.at[role, Y, 0],
            "lo": tok_q.at[role, XY, 0, low],
            "hi": tok_q.at[role, XY, 0, high],
            "plo": diag_q.at[low],
            "phi": diag_q.at[high],
            "px": x_q,
            "py": y_q,
        }[step]

    def source(role, op):
        kind, step = op[0], op[1]
        if kind == "sc":
            if step in ("in", "out"):
                return sc.at[op[2]]
            return {"c": sc.at[role, NONE, 0], "x": sc.at[role, NONE], "y": sc.at[role, pl.ds(0, 2)]}[
                step
            ]
        if kind == "P":
            plane = op[2]
            at = halves(lead, plane)
            low, high = pl.ds(0, at), pl.ds(at, lead - at)
            if step == "c":
                return tok_p.at[plane, op[3], 0]
            if step == "pc":
                return part_p.at[plane, op[3], 1]
            if step in ("in", "out", "x", "y"):
                return tok_p.at[plane, NONE, 0, high if op[3] else low]
            if step in ("px", "py", "rin", "rout"):
                place = {"px": X, "py": Y}.get(step, NONE)
                return part_p.at[plane, place, 0, high if op[3] else low]
            return {
                "lo": tok_p.at[plane, Y, 0, low],
                "hi": tok_p.at[plane, X, 0, high],
                "plo": part_p.at[plane, XY, 0, low],
                "phi": part_p.at[plane, XY, 0, high],
            }[step]
        at = halves(rest, role)
        low, high = pl.ds(0, at), pl.ds(at, rest - at)
        if step in ("in", "out", "c"):
            return tok_q.at[op[2], op[3], 0]
        if step == "pc":
            return part_q.at[op[2], pl.ds(2 * op[3], 2), 1]
        if step in ("rin", "rout"):
            return part_q.at[op[2], op[3], 0]
        return {
            "x": tok_q.at[role, NONE, 0],
            "y": tok_q.at[role, NONE, 0],
            "lo": tok_q.at[role, Y, 0, low],
            "hi": tok_q.at[role, X, 0, high],
            "plo": part_q.at[role, XY, 0, low],
            "phi": part_q.at[role, XY, 0, high],
            "px": part_q.at[role, X, 0],
            "py": part_q.at[role, Y, 0],
        }[step]

    arrived = set()
    sent = {END: [], MID: []}

    def arrive(role, *names):
        for name in names:
            if (role, name) in arrived:
                continue
            arrived.add((role, name))
            ref = landing(role, name)
            pltpu.make_async_remote_copy(
                src_ref=ref,
                dst_ref=ref,
                send_sem=send_sem.at[0],
                recv_sem=recv_sem.at[number(name)],
                device_id=partner["c"],
                device_id_type=MESH,
            ).wait_recv()

    def block_here(role, kind, plane, at):
        if kind == "Q":
            if plane != role:
                return [("Q", "z", plane, at)]
            return {
                NONE: [],
                X: [("Q", "x")],
                Y: [("Q", "y")],
                XY: [("Q", "lo"), ("Q", "hi")],
            }[at]
        if at == XY:
            return [("P", "lo", plane), ("P", "hi", plane)]
        if at == NONE and plane == role:
            return []
        return [("P", ("z", "x", "y")[at], plane, part) for part in range(2)]

    def scales_here(role, plane, at):
        if plane != role:
            return [("sc", "z", plane)]
        return [[("sc", "c")], [("sc", "x")], [("sc", "y")], [("sc", "y")]][at]

    def needs(role, op):
        kind, step = op[0], op[1]
        if kind == "sc":
            if step in ("in", "out"):
                return scales_here(role, op[2], XY)
            return {"c": [], "x": [("sc", "c")], "y": [("sc", "x")]}[step]
        if step == "c":
            return block_here(role, kind, op[2], op[3])
        if step == "lo":
            return [("P", "y", op[2], 0)] if kind == "P" else [("Q", "y")]
        if step == "hi":
            return [("P", "x", op[2], 1)] if kind == "P" else [("Q", "x")]
        if step in ("in", "out", "x", "y"):
            if kind == "P":
                return [] if op[2] == role else [("P", "z", op[2], op[3])]
            return block_here(role, kind, op[2], op[3]) if step in ("in", "out") else []
        return []

    def copy_of(role, op, at):
        link, _, name = target(role, op)
        there = END if link == "out" else MID if link == "in" else role
        return pltpu.make_async_remote_copy(
            src_ref=source(role, op),
            dst_ref=landing(there, name),
            send_sem=send_sem.at[at],
            recv_sem=recv_sem.at[number(name)],
            device_id=partner[link],
            device_id_type=MESH,
        )

    def send(role, op):
        arrive(role, *needs(role, op))
        copy_of(role, op, len(sent[role])).start()
        sent[role].append(op)

    def f32(values):
        return values.astype(jnp.float32)

    def sides(role, plane):
        if role == plane:
            return (0,) if role == END else (1, 0)
        if role == END:
            return ()
        return (0,) if plane == END else (1,)

    def bf16(values):
        return values.astype(jnp.bfloat16)

    def chip_p(role, plane, at, span):
        arrive(role, ("P", "pc", plane, at))
        return f32(part_p[plane, at, 0, span]) + f32(core_p[plane, at, span])

    def chip_q(role, plane, at):
        arrive(role, ("Q", "pc", plane, at // 2))
        total = f32(part_q[plane, at, 0]) + f32(core_q[plane, at])
        for side in sides(role, plane):
            arrive(role, ("Q", "rz", side, plane, at))
            total = total + f32(line_q[side, plane, at])
        return total

    def add_p(role, step, plane, part=None):
        cut = halves(lead, plane)
        span = slice(cut, lead) if part else slice(0, cut)
        if step == "d":
            part_p[plane, XY, 0] = bf16(chip_p(role, plane, XY, slice(0, lead)))
        elif step in ("sx", "sy"):
            at = X if step == "sx" else Y
            total = chip_p(role, plane, at, span)
            if part == (1 if step == "sx" else 0):
                arrive(role, ("P", "phi" if step == "sx" else "plo", plane))
                total = total + f32(diag_p[plane, span])
            part_p[plane, at, 0, span] = bf16(total)
        else:
            total = chip_p(role, plane, NONE, span)
            arrive(role, ("P", "px", plane, part), ("P", "py", plane, part))
            total = total + f32(x_p[plane, span]) + f32(y_p[plane, span])
            for side in sides(role, plane):
                arrive(role, ("P", "rz", side, plane, part))
                total = total + f32(line_p[side, plane, span])
            if plane == role:
                out_ref[span] = total.astype(out_ref.dtype)
            else:
                part_p[plane, NONE, 0, span] = bf16(total)

    def add_q(role, step, *more):
        cut = halves(rest, role)
        if step == "col":
            plane, at = more
            part_q[plane, at, 0] = bf16(chip_q(role, plane, at))
        elif step == "d":
            part_q[role, XY, 0] = bf16(chip_q(role, role, XY))
        elif step == "sx":
            total = chip_q(role, role, X)
            arrive(role, ("Q", "phi"))
            part_q[role, X, 0, :cut] = bf16(total[:cut])
            part_q[role, X, 0, cut:] = bf16(total[cut:] + f32(diag_q[cut:]))
        elif step == "sy":
            total = chip_q(role, role, Y)
            arrive(role, ("Q", "plo"))
            part_q[role, Y, 0, :cut] = bf16(total[:cut] + f32(diag_q[:cut]))
            part_q[role, Y, 0, cut:] = bf16(total[cut:])
        else:
            total = chip_q(role, role, NONE)
            arrive(role, ("Q", "px"), ("Q", "py"))
            out_ref[lead:] = (total + f32(x_q[...]) + f32(y_q[...])).astype(out_ref.dtype)

    def scale_columns(blocks, low, high):
        line = lax.broadcasted_iota(jnp.int32, (high - low, lines), 1)
        routed, shared = [], []
        for block in blocks:
            columns = jnp.transpose(block)[low:high]
            routed.append(jnp.sum(jnp.where(line == e_at, columns, 0.0), axis=1, keepdims=True))
            shared.append(columns[:, lines - 1 :])
        return jnp.concatenate(routed, axis=0), jnp.concatenate(shared, axis=0)

    def experts(inputs, scales):
        routed_scale, shared_scale = scales
        gate_part = jnp.dot(inputs, w_gate[...], preferred_element_type=jnp.float32)
        up_part = jnp.dot(inputs, w_up[...], preferred_element_type=jnp.float32)
        hidden = gate_part * jax.nn.sigmoid(gate_part) * up_part
        hidden = jnp.concatenate(
            [
                bf16(hidden[:, :hidden_units] * routed_scale),
                bf16(hidden[:, hidden_units:] * shared_scale),
            ],
            axis=1,
        )
        return bf16(jnp.dot(hidden, w_down[...], preferred_element_type=jnp.float32))

    def by_role(at_end, at_mid):
        return at_end if at_end == at_mid else at_end + (at_mid - at_end) * mid

    def compute(op_end, op_mid):
        plane, at = by_role(op_end[1], op_mid[1]), by_role(op_end[2], op_mid[2])
        width = tok_p.shape[4]
        if op_end[0] == "CP":
            inputs = tok_p[plane, at].reshape(2 * lead, width)
            blocks = [sc[plane, at, core] for core in range(2)]
            result = experts(inputs, scale_columns(blocks, 0, lead))
            part_p[plane, at] = result.reshape(2, lead, width)
        else:
            pair = pl.ds(2 * at, 2)
            inputs = tok_q[plane, pair].reshape(4 * rest, width)
            blocks = [sc[plane, 2 * at + one, core] for one in range(2) for core in range(2)]
            result = experts(inputs, scale_columns(blocks, lead, rows))
            part_q[plane, pair] = result.reshape(2, 2, rest, width)

    def ready(role, op):
        plane, at = op[1], op[2]
        if op[0] == "CP":
            arrive(role, *block_here(role, "P", plane, at), ("P", "c", plane, at))
            arrive(role, *scales_here(role, plane, at))
        else:
            for one in (2 * at, 2 * at + 1):
                arrive(role, *block_here(role, "Q", plane, one), ("Q", "c", plane, one))
                arrive(role, *scales_here(role, plane, one))

    def anchors(role, order):
        parts, ops = [[]], operations(role)
        for op in (ops[at] for at in order):
            parts[-1].append(op)
            if op[0] in ANCHORS:
                parts.append([])
        return parts

    def run(role, part):
        for op in part:
            if op[0] in ("S", "W"):
                continue
            if op[0] in ("CP", "CQ"):
                ready(role, op)
            elif op[0] == "P" and op[1] in ("d", "sx", "sy", "col"):
                add_p(role, *op[1:])
            elif op[0] == "Q" and op[1] in ("d", "sx", "sy", "col", "end"):
                add_q(role, *op[1:])
            else:
                send(role, op)

    for part_end, part_mid in zip(anchors(END, ORDER_END), anchors(MID, ORDER_MID), strict=True):

        @pl.when(mid == 0)
        def _():
            run(END, part_end)

        @pl.when(mid == 1)
        def _():
            run(MID, part_mid)

        if not part_end or part_end[-1][0] not in ANCHORS:
            continue
        if part_end[-1][0] == "S":
            make_scales()
        elif part_end[-1][0] == "W":
            for load in loads:
                load.wait()
            w_down[0:hidden_units, :] = jnp.transpose(down_raw[...])
        else:
            compute(part_end[-1], part_mid[-1])

    @pl.when(mid == 0)
    def _():
        for at, op in enumerate(sent[END]):
            copy_of(END, op, at).wait_send()

    @pl.when(mid == 1)
    def _():
        for at, op in enumerate(sent[MID]):
            copy_of(MID, op, at).wait_send()


def fused_body(
    tokens,
    norm_gain,
    router_weight,
    shared_gate_vector,
    expert_ids,
    gate_weight,
    up_weight,
    down_weight,
    shared_gate_weight,
    shared_up_weight,
    shared_down_weight,
):
    rows, width = tokens.shape
    hidden_units = gate_weight.shape[2]
    shared_units = shared_gate_weight.shape[1] // lax.axis_size("dp")
    units = hidden_units + shared_units
    lead = LEAD_SHARE * rows // 8
    rest = rows - lead
    anywhere = pl.BlockSpec(memory_space=pl.ANY)

    def blocks(count, *planes):
        return pltpu.VMEM(planes + (count, width), jnp.bfloat16)

    return pl.pallas_call(
        functools.partial(fused_kernel, rows, lead, hidden_units, shared_units),
        out_shape=jax.ShapeDtypeStruct((rows, width), jnp.bfloat16),
        in_specs=[anywhere] * 11,
        out_specs=pl.BlockSpec(memory_space=pltpu.VMEM),
        scratch_shapes=[
            blocks(rows),
            pltpu.VMEM(norm_gain.shape, norm_gain.dtype),
            pltpu.VMEM(router_weight.shape[::-1], router_weight.dtype),
            pltpu.VMEM(shared_gate_vector.shape, shared_gate_vector.dtype),
            pltpu.VMEM(expert_ids.shape[::-1], expert_ids.dtype),
            pltpu.VMEM((4, 4, 2, 8, rows), jnp.float32),
            blocks(lead, 4, 4, 2),
            blocks(rest, 4, 4, 2),
            blocks(lead, 4, 4, 2),
            blocks(rest, 4, 4, 2),
            blocks(lead, 4, 4),
            blocks(rest, 4, 4),
            blocks(lead, 4),
            blocks(rest),
            blocks(lead, 4),
            blocks(rest),
            blocks(lead, 4),
            blocks(rest),
            blocks(lead, 2, 4),
            blocks(rest, 2, 4, 4),
            pltpu.VMEM((width, units), jnp.bfloat16),
            pltpu.VMEM((width, units), jnp.bfloat16),
            pltpu.VMEM((width, hidden_units), jnp.bfloat16),
            pltpu.VMEM((units, width), jnp.bfloat16),
            pltpu.SemaphoreType.DMA((SEMAPHORES,)),
            pltpu.SemaphoreType.DMA((SEMAPHORES,)),
            pltpu.SemaphoreType.DMA((11,)),
        ],
        compiler_params=pltpu.CompilerParams(
            collective_id=0, has_side_effects=True, vmem_limit_bytes=VMEM_LIMIT
        ),
    )(
        tokens,
        norm_gain,
        router_weight.T,
        shared_gate_vector,
        expert_ids.T,
        gate_weight,
        up_weight,
        down_weight,
        shared_gate_weight,
        shared_up_weight,
        shared_down_weight,
    )


def solution(mesh):
    fused = (mesh.shape["expert"], mesh.shape["dp"]) == (1 << 2, 1 << 3)
    return jax.shard_map(
        fused_body if fused else body,
        mesh=mesh,
        in_specs=(
            P(("expert", "dp"), None),
            P(),
            P(),
            P(),
            P(("expert", "dp"), None),
            P("expert", None, "dp"),
            P("expert", None, "dp"),
            P("expert", None, "dp"),
            P(None, "expert"),
            P(None, "expert"),
            P("expert", None),
        ),
        out_specs=P(("expert", "dp"), None),
        check_vma=False,
    )
```

```python
import functools

import jax
import jax.numpy as jnp
from jax import lax
from jax.experimental import pallas as pl
from jax.experimental.pallas import tpu as pltpu
from jax.sharding import PartitionSpec as P


def rms_norm(values, gain):
    floats = values.astype(jnp.float32)
    mean_square = jnp.mean(floats * floats, axis=-1, keepdims=True)
    return (floats * lax.rsqrt(mean_square + 1e-06) * gain).astype(jnp.bfloat16)


def routing(normed, router_weight, expert_ids):
    logits = jnp.dot(normed, router_weight, preferred_element_type=jnp.float32)
    onehot = (
        expert_ids[:, :, None] == jnp.arange(router_weight.shape[1], dtype=jnp.int32)[None, None, :]
    )
    picked = jnp.sum(jnp.where(onehot, logits[:, None, :], jnp.float32(0.0)), axis=-1)
    first_weight = jax.nn.sigmoid(picked[:, 0] - picked[:, 1])
    return jnp.stack([first_weight, 1.0 - first_weight], axis=1)


def slot_of(block_ids, experts):
    flat_ids = block_ids.reshape(-1)
    onehot = (flat_ids[:, None] == jnp.arange(experts, dtype=jnp.int32)[None, :]).astype(jnp.int32)
    before = jnp.cumsum(onehot, axis=0) - onehot
    return jnp.sum(before * onehot, axis=1).reshape(block_ids.shape)


def swiglu_hidden(inputs, gate_piece, up_piece):
    gate_part = jnp.dot(inputs, gate_piece, preferred_element_type=jnp.float32)
    up_part = jnp.dot(inputs, up_piece, preferred_element_type=jnp.float32)
    return (jax.nn.silu(gate_part) * up_part).astype(jnp.bfloat16)


def down_product(hidden, down_piece):
    return lax.dot_general(
        hidden, down_piece, (((1,), (1,)), ((), ())), preferred_element_type=jnp.float32
    )


def body(
    tokens,
    norm_gain,
    router_weight,
    shared_gate_vector,
    expert_ids,
    gate_weight,
    up_weight,
    down_weight,
    shared_gate_weight,
    shared_up_weight,
    shared_down_weight,
):
    experts = lax.axis_size("expert")
    tok_rows = tokens.shape[0]
    width = tokens.shape[1]
    capacity = 3 * tok_rows // experts
    normed = rms_norm(tokens, norm_gain)
    route_weight = routing(normed, router_weight, expert_ids)
    slot = slot_of(expert_ids, experts)
    target = expert_ids * capacity + slot
    slot_iota = jnp.arange(experts * capacity, dtype=jnp.int32)[:, None]
    dispatch_table = (
        (target[:, 0][None, :] == slot_iota) | (target[:, 1][None, :] == slot_iota)
    ).astype(jnp.bfloat16)
    outgoing = jnp.dot(dispatch_table, normed, preferred_element_type=jnp.float32).astype(
        jnp.bfloat16
    )
    outgoing = outgoing.reshape(experts, capacity, width)
    arrived = lax.all_to_all(outgoing, "expert", split_axis=0, concat_axis=0, tiled=True).reshape(
        experts * capacity, width
    )
    hidden = swiglu_hidden(
        arrived,
        lax.all_gather(gate_weight, "dp", axis=2, tiled=True)[0],
        lax.all_gather(up_weight, "dp", axis=2, tiled=True)[0],
    )
    hidden_all = hidden
    hidden = hidden_all
    expert_out = down_product(hidden, lax.all_gather(down_weight, "dp", axis=2, tiled=True)[0])
    expert_out = expert_out.astype(jnp.bfloat16).reshape(experts, capacity, width)
    returned_rows = lax.all_to_all(
        expert_out, "expert", split_axis=0, concat_axis=0, tiled=True
    ).reshape(experts * capacity, width)
    fetched = returned_rows[target].astype(jnp.float32)
    routed = jnp.sum(route_weight[:, :, None] * fetched, axis=1)
    gathered = lax.all_gather(normed, "expert", axis=0, tiled=True)
    hidden = swiglu_hidden(gathered, shared_gate_weight, shared_up_weight)
    shared = lax.psum_scatter(
        jnp.dot(hidden, shared_down_weight, preferred_element_type=jnp.float32).astype(
            jnp.bfloat16
        ),
        "expert",
        scatter_dimension=0,
        tiled=True,
    ).astype(jnp.float32)
    shared_gate = jax.nn.sigmoid(jnp.sum(normed.astype(jnp.float32) * shared_gate_vector, axis=-1))
    return (routed + shared_gate[:, None] * shared).astype(jnp.bfloat16)

MESH = pl.DeviceIdType.MESH
NONE, X, Y, XY = 0, 1, 2, 3
END, MID = 0, 1
VMEM_LIMIT = 62 * 1024 * 1024
SEMAPHORES = 192
LEAD_SHARE = 6
ANCHORS = ("S", "W", "CP", "CQ")


def operations(role):
    ops = [("S",), ("W",), ("sc", "c"), ("sc", "x"), ("sc", "y")]
    travels = [("in", 0)] if role == 0 else [("out", 1), ("in", 1), ("in", 0), ("out", 2), ("out", 3)]
    returns = [("rin", 1), ("rin", 2), ("rin", 3)] if role == 0 else [("rout", 0), ("rin", 2), ("rin", 3)]
    ops += [("sc",) + way for way in travels]
    ops += [("P",) + way + (half,) for way in travels + returns for half in range(2)]
    for plane in range(4):
        ops += [
            ("P", step, plane, half) for step in ("x", "y", "sx", "sy", "px", "py", "col") for half in range(2)
        ]
        ops += [("P", step, plane) for step in ("lo", "hi", "d", "plo", "phi")]
        ops += [(kind, *step, plane, at) for kind, *step in (("P", "c"), ("CP",), ("P", "pc")) for at in range(4)]
        ops += [(kind, *step, plane, pair) for kind, *step in (("CQ",), ("Q", "pc")) for pair in range(2)]
        ops += [("Q", "c", plane, at) for at in range(4)]
        if plane != role:
            ops += [("Q", "col", plane, at) for at in range(4)]
    ops += [("Q",) + way + (at,) for way in travels + returns for at in range(4)]
    ops += [("Q", step) for step in ("x", "y", "lo", "hi", "d", "plo", "phi", "sx", "px", "sy", "py", "end")]
    return ops


ORDER_END = (
    6, 49, 198, 199, 33, 0, 15, 7, 2, 16, 1, 200, 3, 201, 184, 55,
    53, 51, 183, 50, 29, 72, 54, 182, 52, 45, 4, 185, 67, 47, 37, 98,
    41, 115, 97, 73, 68, 5, 46, 139, 48, 141, 133, 110, 111, 158, 75, 140,
    142, 176, 153, 134, 99, 118, 177, 96, 159, 154, 160, 171, 173, 175, 163, 167,
    117, 28, 56, 181, 174, 197, 180, 164, 168, 196, 143, 147, 128, 161, 90, 116,
    130, 17, 170, 172, 146, 122, 91, 126, 150, 74, 14, 36, 138, 193, 179, 131,
    137, 178, 165, 169, 195, 35, 112, 113, 132, 114, 40, 192, 44, 155, 157, 156,
    34, 85, 87, 88, 194, 127, 129, 89, 30, 31, 32, 95, 189, 94, 162, 166,
    188, 136, 191, 202, 135, 84, 86, 203, 204, 144, 148, 190, 145, 149, 79, 83,
    93, 92, 121, 125, 186, 69, 70, 71, 207, 120, 103, 205, 124, 208, 206, 187,
    152, 151, 102, 119, 13, 106, 123, 100, 104, 101, 77, 12, 105, 107, 81, 78,
    82, 209, 76, 80, 108, 10, 57, 61, 58, 59, 63, 60, 39, 62, 64, 43,
    109, 11, 38, 42, 20, 21, 24, 65, 8, 18, 22, 19, 23, 25, 66, 9,
    26, 27,
)
ORDER_MID = (
    227, 12, 226, 10, 104, 88, 0, 2, 13, 11, 71, 70, 1, 14, 3, 228,
    229, 28, 16, 106, 26, 105, 200, 110, 127, 45, 17, 27, 100, 15, 63, 107,
    102, 92, 18, 4, 153, 96, 109, 62, 204, 201, 145, 61, 208, 40, 46, 41,
    170, 64, 19, 101, 205, 152, 103, 123, 188, 203, 212, 58, 7, 165, 209, 154,
    48, 146, 60, 50, 202, 189, 213, 54, 49, 6, 166, 122, 187, 198, 53, 57,
    9, 211, 30, 59, 151, 83, 172, 183, 84, 199, 186, 185, 52, 210, 173, 130,
    29, 56, 176, 8, 196, 180, 177, 181, 171, 197, 108, 111, 144, 143, 42, 158,
    140, 167, 142, 206, 182, 168, 169, 184, 91, 47, 134, 207, 138, 193, 129, 225,
    128, 69, 72, 139, 5, 141, 192, 194, 224, 124, 175, 157, 179, 162, 195, 43,
    132, 136, 68, 217, 150, 221, 155, 161, 159, 89, 90, 156, 67, 133, 216, 137,
    191, 223, 112, 94, 160, 98, 149, 44, 220, 115, 174, 178, 119, 76, 125, 66,
    190, 215, 222, 51, 55, 230, 131, 126, 231, 34, 135, 31, 32, 33, 65, 214,
    93, 232, 97, 148, 35, 219, 36, 114, 95, 99, 147, 218, 113, 235, 73, 118,
    116, 85, 233, 37, 117, 164, 25, 87, 86, 163, 24, 236, 234, 39, 21, 120,
    22, 80, 77, 74, 75, 38, 121, 20, 23, 79, 78, 237, 82, 81,
)


def flipped(position, bit):
    return position + bit - 2 * bit * ((position // bit) % 2)


def halves(count, number):
    half = count // 2 // 16 * 16
    if 2 * half == count or number in (1, 2):
        return half
    return count - half


def target(role, op):
    kind, step, rest = op[0], op[1], op[2:]
    if step in ("in", "out"):
        plane, more = rest[0], rest[1:]
        if step == "out":
            return "out", END, (kind, "z", plane) + more
        return "in", MID, (kind, "z", plane if role == END else 3 - plane) + more
    if step == "rin":
        plane, more = rest[0], rest[1:]
        if role == END:
            return "in", MID, (kind, "rz", 1, plane) + more
        return "in", MID, (kind, "rz", 0, 3 - plane) + more
    if step == "rout":
        return "out", END, (kind, "rz", 0) + rest
    if step in ("c", "pc"):
        return "c", role, op
    return ("x" if step in ("x", "lo", "plo", "px") else "y"), role, op


def fused_kernel(
    rows,
    lead,
    hidden_units,
    shared_units,
    tokens_in,
    gain_in,
    router_in,
    vector_in,
    ids_in,
    gate_ref,
    up_ref,
    down_ref,
    sgate_ref,
    sup_ref,
    sdown_ref,
    out_ref,
    tokens_ref,
    gain_ref,
    router_ref,
    vector_ref,
    ids_ref,
    sc,
    tok_p,
    tok_q,
    part_p,
    part_q,
    core_p,
    core_q,
    diag_p,
    diag_q,
    x_p,
    x_q,
    y_p,
    y_q,
    line_p,
    line_q,
    w_gate,
    w_up,
    down_raw,
    w_down,
    send_sem,
    recv_sem,
    load_sem,
):
    e_at = lax.axis_index("expert")
    d_at = lax.axis_index("dp")
    rest = rows - lead
    z_at = d_at // 2
    toward = 2 * (1 - 2 * (z_at // 2))
    mid = (z_at + z_at // 2) % 2
    partner = {
        "c": (flipped(e_at, 1), d_at),
        "x": (flipped(e_at, 2), d_at),
        "y": (e_at, flipped(d_at, 1)),
        "in": (e_at, d_at + toward),
        "out": (e_at, d_at - toward),
    }
    barrier = pltpu.get_barrier_semaphore()
    for to in ("c", "x", "y", "in"):
        pl.semaphore_signal(barrier, inc=1, device_id=partner[to], device_id_type=MESH)

    @pl.when(mid == 1)
    def _():
        pl.semaphore_signal(barrier, inc=1, device_id=partner["out"], device_id_type=MESH)

    inputs = [
        pltpu.make_async_copy(there, here, load_sem.at[6 + at])
        for at, (there, here) in enumerate(
            (
                (tokens_in, tokens_ref),
                (gain_in, gain_ref),
                (router_in, router_ref),
                (vector_in, vector_ref),
                (ids_in, ids_ref),
            )
        )
    ]
    for load in inputs:
        load.start()

    first = pl.multiple_of(d_at * shared_units, shared_units)
    loads = [
        pltpu.make_async_copy(gate_ref.at[0], w_gate.at[:, pl.ds(0, hidden_units)], load_sem.at[0]),
        pltpu.make_async_copy(up_ref.at[0], w_up.at[:, pl.ds(0, hidden_units)], load_sem.at[1]),
        pltpu.make_async_copy(
            sgate_ref.at[:, pl.ds(first, shared_units)],
            w_gate.at[:, pl.ds(hidden_units, shared_units)],
            load_sem.at[2],
        ),
        pltpu.make_async_copy(
            sup_ref.at[:, pl.ds(first, shared_units)],
            w_up.at[:, pl.ds(hidden_units, shared_units)],
            load_sem.at[3],
        ),
        pltpu.make_async_copy(
            sdown_ref.at[pl.ds(first, shared_units), :],
            w_down.at[pl.ds(hidden_units, shared_units), :],
            load_sem.at[4],
        ),
        pltpu.make_async_copy(down_ref.at[0], down_raw, load_sem.at[5]),
    ]
    for load in loads:
        load.start()
    for load in inputs:
        load.wait()

    floats = tokens_ref[...].astype(jnp.float32)
    mean_square = jnp.mean(floats * floats, axis=-1, keepdims=True)
    normed = (floats * lax.rsqrt(mean_square + 1e-06) * gain_ref[...][None, :]).astype(jnp.bfloat16)
    tok_p[mid, NONE, 0] = normed[:lead]
    tok_q[mid, NONE, 0] = normed[lead:]
    pl.semaphore_wait(barrier, 4 + mid)

    lines = sc.shape[3]
    def make_scales():
        normed = jnp.concatenate([tok_p[mid, NONE, 0], tok_q[mid, NONE, 0]], axis=0)
        logits = lax.dot_general(
            router_ref[...], normed, (((1,), (1,)), ((), ())), preferred_element_type=jnp.float32
        )
        ids = ids_ref[...]
        first_id, second_id = ids[0:1], ids[1:2]
        row = lax.broadcasted_iota(jnp.int32, logits.shape, 0)
        margin = jnp.sum(
            jnp.where(row == first_id, logits, 0.0), axis=0, keepdims=True
        ) - jnp.sum(jnp.where(row == second_id, logits, 0.0), axis=0, keepdims=True)
        first_weight = jax.nn.sigmoid(margin)
        shared_gate = jax.nn.sigmoid(
            jnp.sum(normed.astype(jnp.float32) * vector_ref[...][None, :], axis=-1, keepdims=True)
        )
        column = lax.broadcasted_iota(jnp.int32, (rows, lines), 1)
        row = lax.broadcasted_iota(jnp.int32, (lines, rows), 0)
        scales = jnp.transpose(jnp.where(column == lines - 1, shared_gate, 0.0))
        scales = scales + jnp.where(row == first_id, first_weight, 0.0)
        scales = scales + jnp.where(row == second_id, 1.0 - first_weight, 0.0)
        sc[mid, NONE, 0] = scales

    numbers = {}

    def number(name):
        return numbers.setdefault(name, len(numbers))

    def landing(role, name):
        kind, step = name[0], name[1]
        if kind == "sc":
            if step == "z":
                return sc.at[name[2]]
            return {"c": sc.at[role, NONE, 1], "x": sc.at[role, X], "y": sc.at[role, pl.ds(2, 2)]}[step]
        if kind == "P":
            plane = name[3] if step == "rz" else name[2]
            at = halves(lead, plane)
            low, high = pl.ds(0, at), pl.ds(at, lead - at)
            if step == "rz":
                return line_p.at[name[2], plane, high if name[4] else low]
            if step == "c":
                return tok_p.at[plane, name[3], 1]
            if step == "pc":
                return core_p.at[plane, name[3]]
            if step in ("z", "x", "y"):
                place = {"z": NONE, "x": X, "y": Y}[step]
                return tok_p.at[plane, place, 0, high if name[3] else low]
            if step in ("px", "py"):
                return (x_p if step == "px" else y_p).at[plane, high if name[3] else low]
            return {
                "lo": tok_p.at[plane, XY, 0, low],
                "hi": tok_p.at[plane, XY, 0, high],
                "plo": diag_p.at[plane, low],
                "phi": diag_p.at[plane, high],
            }[step]
        at = halves(rest, role)
        low, high = pl.ds(0, at), pl.ds(at, rest - at)
        if step == "rz":
            return line_q.at[name[2], name[3], name[4]]
        if step == "z":
            return tok_q.at[name[2], name[3], 0]
        if step == "c":
            return tok_q.at[name[2], name[3], 1]
        if step == "pc":
            return core_q.at[name[2], pl.ds(2 * name[3], 2)]
        return {
            "x": tok_q.at[role, X, 0],
            "y": tok_q.at[role, Y, 0],
            "lo": tok_q.at[role, XY, 0, low],
            "hi": tok_q.at[role, XY, 0, high],
            "plo": diag_q.at[low],
            "phi": diag_q.at[high],
            "px": x_q,
            "py": y_q,
        }[step]

    def source(role, op):
        kind, step = op[0], op[1]
        if kind == "sc":
            if step in ("in", "out"):
                return sc.at[op[2]]
            return {"c": sc.at[role, NONE, 0], "x": sc.at[role, NONE], "y": sc.at[role, pl.ds(0, 2)]}[
                step
            ]
        if kind == "P":
            plane = op[2]
            at = halves(lead, plane)
            low, high = pl.ds(0, at), pl.ds(at, lead - at)
            if step == "c":
                return tok_p.at[plane, op[3], 0]
            if step == "pc":
                return part_p.at[plane, op[3], 1]
            if step in ("in", "out", "x", "y"):
                return tok_p.at[plane, NONE, 0, high if op[3] else low]
            if step in ("px", "py", "rin", "rout"):
                place = {"px": X, "py": Y}.get(step, NONE)
                return part_p.at[plane, place, 0, high if op[3] else low]
            return {
                "lo": tok_p.at[plane, Y, 0, low],
                "hi": tok_p.at[plane, X, 0, high],
                "plo": part_p.at[plane, XY, 0, low],
                "phi": part_p.at[plane, XY, 0, high],
            }[step]
        at = halves(rest, role)
        low, high = pl.ds(0, at), pl.ds(at, rest - at)
        if step in ("in", "out", "c"):
            return tok_q.at[op[2], op[3], 0]
        if step == "pc":
            return part_q.at[op[2], pl.ds(2 * op[3], 2), 1]
        if step in ("rin", "rout"):
            return part_q.at[op[2], op[3], 0]
        return {
            "x": tok_q.at[role, NONE, 0],
            "y": tok_q.at[role, NONE, 0],
            "lo": tok_q.at[role, Y, 0, low],
            "hi": tok_q.at[role, X, 0, high],
            "plo": part_q.at[role, XY, 0, low],
            "phi": part_q.at[role, XY, 0, high],
            "px": part_q.at[role, X, 0],
            "py": part_q.at[role, Y, 0],
        }[step]

    arrived = set()
    sent = {END: [], MID: []}

    def arrive(role, *names):
        for name in names:
            if (role, name) in arrived:
                continue
            arrived.add((role, name))
            ref = landing(role, name)
            pltpu.make_async_remote_copy(
                src_ref=ref,
                dst_ref=ref,
                send_sem=send_sem.at[0],
                recv_sem=recv_sem.at[number(name)],
                device_id=partner["c"],
                device_id_type=MESH,
            ).wait_recv()

    def block_here(role, kind, plane, at):
        if kind == "Q":
            if plane != role:
                return [("Q", "z", plane, at)]
            return {
                NONE: [],
                X: [("Q", "x")],
                Y: [("Q", "y")],
                XY: [("Q", "lo"), ("Q", "hi")],
            }[at]
        if at == XY:
            return [("P", "lo", plane), ("P", "hi", plane)]
        if at == NONE and plane == role:
            return []
        return [("P", ("z", "x", "y")[at], plane, part) for part in range(2)]

    def scales_here(role, plane, at):
        if plane != role:
            return [("sc", "z", plane)]
        return [[("sc", "c")], [("sc", "x")], [("sc", "y")], [("sc", "y")]][at]

    def needs(role, op):
        kind, step = op[0], op[1]
        if kind == "sc":
            if step in ("in", "out"):
                return scales_here(role, op[2], XY)
            return {"c": [], "x": [("sc", "c")], "y": [("sc", "x")]}[step]
        if step == "c":
            return block_here(role, kind, op[2], op[3])
        if step == "lo":
            return [("P", "y", op[2], 0)] if kind == "P" else [("Q", "y")]
        if step == "hi":
            return [("P", "x", op[2], 1)] if kind == "P" else [("Q", "x")]
        if step in ("in", "out", "x", "y"):
            if kind == "P":
                return [] if op[2] == role else [("P", "z", op[2], op[3])]
            return block_here(role, kind, op[2], op[3]) if step in ("in", "out") else []
        return []

    def copy_of(role, op, at):
        link, _, name = target(role, op)
        there = END if link == "out" else MID if link == "in" else role
        return pltpu.make_async_remote_copy(
            src_ref=source(role, op),
            dst_ref=landing(there, name),
            send_sem=send_sem.at[at],
            recv_sem=recv_sem.at[number(name)],
            device_id=partner[link],
            device_id_type=MESH,
        )

    def send(role, op):
        arrive(role, *needs(role, op))
        copy_of(role, op, len(sent[role])).start()
        sent[role].append(op)

    def f32(values):
        return values.astype(jnp.float32)

    def sides(role, plane):
        if role == plane:
            return (0,) if role == END else (1, 0)
        if role == END:
            return ()
        return (0,) if plane == END else (1,)

    def bf16(values):
        return values.astype(jnp.bfloat16)

    def chip_p(role, plane, at, span):
        arrive(role, ("P", "pc", plane, at))
        return f32(part_p[plane, at, 0, span]) + f32(core_p[plane, at, span])

    def chip_q(role, plane, at):
        arrive(role, ("Q", "pc", plane, at // 2))
        total = f32(part_q[plane, at, 0]) + f32(core_q[plane, at])
        for side in sides(role, plane):
            arrive(role, ("Q", "rz", side, plane, at))
            total = total + f32(line_q[side, plane, at])
        return total

    def add_p(role, step, plane, part=None):
        cut = halves(lead, plane)
        span = slice(cut, lead) if part else slice(0, cut)
        if step == "d":
            part_p[plane, XY, 0] = bf16(chip_p(role, plane, XY, slice(0, lead)))
        elif step in ("sx", "sy"):
            at = X if step == "sx" else Y
            total = chip_p(role, plane, at, span)
            if part == (1 if step == "sx" else 0):
                arrive(role, ("P", "phi" if step == "sx" else "plo", plane))
                total = total + f32(diag_p[plane, span])
            part_p[plane, at, 0, span] = bf16(total)
        else:
            total = chip_p(role, plane, NONE, span)
            arrive(role, ("P", "px", plane, part), ("P", "py", plane, part))
            total = total + f32(x_p[plane, span]) + f32(y_p[plane, span])
            for side in sides(role, plane):
                arrive(role, ("P", "rz", side, plane, part))
                total = total + f32(line_p[side, plane, span])
            if plane == role:
                out_ref[span] = total.astype(out_ref.dtype)
            else:
                part_p[plane, NONE, 0, span] = bf16(total)

    def add_q(role, step, *more):
        cut = halves(rest, role)
        if step == "col":
            plane, at = more
            part_q[plane, at, 0] = bf16(chip_q(role, plane, at))
        elif step == "d":
            part_q[role, XY, 0] = bf16(chip_q(role, role, XY))
        elif step == "sx":
            total = chip_q(role, role, X)
            arrive(role, ("Q", "phi"))
            part_q[role, X, 0, :cut] = bf16(total[:cut])
            part_q[role, X, 0, cut:] = bf16(total[cut:] + f32(diag_q[cut:]))
        elif step == "sy":
            total = chip_q(role, role, Y)
            arrive(role, ("Q", "plo"))
            part_q[role, Y, 0, :cut] = bf16(total[:cut] + f32(diag_q[:cut]))
            part_q[role, Y, 0, cut:] = bf16(total[cut:])
        else:
            total = chip_q(role, role, NONE)
            arrive(role, ("Q", "px"), ("Q", "py"))
            out_ref[lead:] = (total + f32(x_q[...]) + f32(y_q[...])).astype(out_ref.dtype)

    def scale_columns(blocks, low, high):
        line = lax.broadcasted_iota(jnp.int32, (high - low, lines), 1)
        routed, shared = [], []
        for block in blocks:
            columns = jnp.transpose(block)[low:high]
            routed.append(jnp.sum(jnp.where(line == e_at, columns, 0.0), axis=1, keepdims=True))
            shared.append(columns[:, lines - 1 :])
        return jnp.concatenate(routed, axis=0), jnp.concatenate(shared, axis=0)

    def experts(inputs, scales):
        routed_scale, shared_scale = scales
        gate_part = jnp.dot(inputs, w_gate[...], preferred_element_type=jnp.float32)
        up_part = jnp.dot(inputs, w_up[...], preferred_element_type=jnp.float32)
        hidden = gate_part * jax.nn.sigmoid(gate_part) * up_part
        hidden = jnp.concatenate(
            [
                bf16(hidden[:, :hidden_units] * routed_scale),
                bf16(hidden[:, hidden_units:] * shared_scale),
            ],
            axis=1,
        )
        return bf16(jnp.dot(hidden, w_down[...], preferred_element_type=jnp.float32))

    def by_role(at_end, at_mid):
        return at_end if at_end == at_mid else at_end + (at_mid - at_end) * mid

    def compute(op_end, op_mid):
        plane, at = by_role(op_end[1], op_mid[1]), by_role(op_end[2], op_mid[2])
        width = tok_p.shape[4]
        if op_end[0] == "CP":
            inputs = tok_p[plane, at].reshape(2 * lead, width)
            blocks = [sc[plane, at, core] for core in range(2)]
            result = experts(inputs, scale_columns(blocks, 0, lead))
            part_p[plane, at] = result.reshape(2, lead, width)
        else:
            pair = pl.ds(2 * at, 2)
            inputs = tok_q[plane, pair].reshape(4 * rest, width)
            blocks = [sc[plane, 2 * at + one, core] for one in range(2) for core in range(2)]
            result = experts(inputs, scale_columns(blocks, lead, rows))
            part_q[plane, pair] = result.reshape(2, 2, rest, width)

    def ready(role, op):
        plane, at = op[1], op[2]
        if op[0] == "CP":
            arrive(role, *block_here(role, "P", plane, at), ("P", "c", plane, at))
            arrive(role, *scales_here(role, plane, at))
        else:
            for one in (2 * at, 2 * at + 1):
                arrive(role, *block_here(role, "Q", plane, one), ("Q", "c", plane, one))
                arrive(role, *scales_here(role, plane, one))

    def anchors(role, order):
        parts, ops = [[]], operations(role)
        for op in (ops[at] for at in order):
            parts[-1].append(op)
            if op[0] in ANCHORS:
                parts.append([])
        return parts

    def run(role, part):
        for op in part:
            if op[0] in ("S", "W"):
                continue
            if op[0] in ("CP", "CQ"):
                ready(role, op)
            elif op[0] == "P" and op[1] in ("d", "sx", "sy", "col"):
                add_p(role, *op[1:])
            elif op[0] == "Q" and op[1] in ("d", "sx", "sy", "col", "end"):
                add_q(role, *op[1:])
            else:
                send(role, op)

    for part_end, part_mid in zip(anchors(END, ORDER_END), anchors(MID, ORDER_MID), strict=True):

        @pl.when(mid == 0)
        def _():
            run(END, part_end)

        @pl.when(mid == 1)
        def _():
            run(MID, part_mid)

        if not part_end or part_end[-1][0] not in ANCHORS:
            continue
        if part_end[-1][0] == "S":
            make_scales()
        elif part_end[-1][0] == "W":
            for load in loads:
                load.wait()
            w_down[0:hidden_units, :] = jnp.transpose(down_raw[...])
        else:
            compute(part_end[-1], part_mid[-1])

    @pl.when(mid == 0)
    def _():
        for at, op in enumerate(sent[END]):
            copy_of(END, op, at).wait_send()

    @pl.when(mid == 1)
    def _():
        for at, op in enumerate(sent[MID]):
            copy_of(MID, op, at).wait_send()


def fused_body(
    tokens,
    norm_gain,
    router_weight,
    shared_gate_vector,
    expert_ids,
    gate_weight,
    up_weight,
    down_weight,
    shared_gate_weight,
    shared_up_weight,
    shared_down_weight,
):
    rows, width = tokens.shape
    hidden_units = gate_weight.shape[2]
    shared_units = shared_gate_weight.shape[1] // lax.axis_size("dp")
    units = hidden_units + shared_units
    lead = LEAD_SHARE * rows // 8
    rest = rows - lead
    anywhere = pl.BlockSpec(memory_space=pl.ANY)

    def blocks(count, *planes):
        return pltpu.VMEM(planes + (count, width), jnp.bfloat16)

    return pl.pallas_call(
        functools.partial(fused_kernel, rows, lead, hidden_units, shared_units),
        out_shape=jax.ShapeDtypeStruct((rows, width), jnp.bfloat16),
        in_specs=[anywhere] * 11,
        out_specs=pl.BlockSpec(memory_space=pltpu.VMEM),
        scratch_shapes=[
            blocks(rows),
            pltpu.VMEM(norm_gain.shape, norm_gain.dtype),
            pltpu.VMEM(router_weight.shape[::-1], router_weight.dtype),
            pltpu.VMEM(shared_gate_vector.shape, shared_gate_vector.dtype),
            pltpu.VMEM(expert_ids.shape[::-1], expert_ids.dtype),
            pltpu.VMEM((4, 4, 2, 8, rows), jnp.float32),
            blocks(lead, 4, 4, 2),
            blocks(rest, 4, 4, 2),
            blocks(lead, 4, 4, 2),
            blocks(rest, 4, 4, 2),
            blocks(lead, 4, 4),
            blocks(rest, 4, 4),
            blocks(lead, 4),
            blocks(rest),
            blocks(lead, 4),
            blocks(rest),
            blocks(lead, 4),
            blocks(rest),
            blocks(lead, 2, 4),
            blocks(rest, 2, 4, 4),
            pltpu.VMEM((width, units), jnp.bfloat16),
            pltpu.VMEM((width, units), jnp.bfloat16),
            pltpu.VMEM((width, hidden_units), jnp.bfloat16),
            pltpu.VMEM((units, width), jnp.bfloat16),
            pltpu.SemaphoreType.DMA((SEMAPHORES,)),
            pltpu.SemaphoreType.DMA((SEMAPHORES,)),
            pltpu.SemaphoreType.DMA((11,)),
        ],
        compiler_params=pltpu.CompilerParams(
            collective_id=0, has_side_effects=True, vmem_limit_bytes=VMEM_LIMIT
        ),
    )(
        tokens,
        norm_gain,
        router_weight.T,
        shared_gate_vector,
        expert_ids.T,
        gate_weight,
        up_weight,
        down_weight,
        shared_gate_weight,
        shared_up_weight,
        shared_down_weight,
    )


def solution(mesh):
    fused = (mesh.shape["expert"], mesh.shape["dp"]) == (1 << 2, 1 << 3)
    return jax.shard_map(
        fused_body if fused else body,
        mesh=mesh,
        in_specs=(
            P(("expert", "dp"), None),
            P(),
            P(),
            P(),
            P(("expert", "dp"), None),
            P("expert", None, "dp"),
            P("expert", None, "dp"),
            P("expert", None, "dp"),
            P(None, "expert"),
            P(None, "expert"),
            P("expert", None),
        ),
        out_specs=P(("expert", "dp"), None),
        check_vma=False,
    )
```
